128 devices in a mesh: rows: 4 (over z), cols: 8 (over y_hi, x), slabs: 4 (over y_lo, core).
Axes of the slice: x: 4, y: 4 (y_hi: 2, y_lo: 2; y = y_hi * 2 + y_lo), z: 4, core: 2. Of those that a mesh axis runs over, the one named last changes fastest.
Arguments:
- tracer: float32 [16, 512, 256, 128], P('rows', 'cols', 'slabs'), may hold values from 0.2 to 1.8
- crowding: float32 [16, 512, 256, 128], P('rows', 'cols', 'slabs'), may hold values from 0.5 to 2
Outputs:
- column_sum: float32 [16, 512, 256, 128], P('rows', 'cols', 'slabs')
- tracer_end: float32 [16, 512, 256, 128], P('rows', 'cols', 'slabs')
The draws below stay inside these ranges and needn't reach their ends.
All inputs are finite; a program needn't handle non-finite values.
Results may differ from the reference program's by a relative error of at most 0.00002.
Values sent between devices are 32-bit elements; how exact they have to be, the bound alone decides.
A program may use at most 320 MiB of HBM per device.

```python
import jax
import jax.numpy as jnp
from jax import lax

GRID_Y = 16
GRID_X = 512
GRID_Z = 256
LEVELS = 128
STEPS = 4


def shard_levels(own_key, shape, cuts, low, top_value):
    def one(dim, shards_of):
        steps = jax.random.uniform(jax.random.fold_in(jax.random.fold_in(own_key, 6), dim), (shards_of,), jnp.float32, low / len(cuts), top_value / len(cuts))
        return jnp.repeat(jnp.exp(steps), shape[dim] // shards_of).reshape((-1,) + (1,) * (len(shape) - dim - 1))

    factor_of = one(*cuts[0])
    for cut in cuts[1:]:
        factor_of = factor_of * one(*cut)
    return factor_of


def setup_inputs(seed: int = 0) -> dict:
    splits = jax.random.split(jax.random.key(seed), 3)
    tracer = jnp.clip(0.2 + 1.5999999 * jax.random.uniform(splits[0], (GRID_Y, GRID_X, GRID_Z, LEVELS), jnp.float32) ** shard_levels(splits[0], (GRID_Y, GRID_X, GRID_Z, LEVELS), ((0, 4), (1, 8), (2, 4)), -0.2, 0.2), 0.2, 1.8)
    crowding = jnp.clip(0.5 + 1.5 * jax.random.uniform(splits[1], (GRID_Y, GRID_X, GRID_Z, LEVELS), jnp.float32) ** shard_levels(splits[1], (GRID_Y, GRID_X, GRID_Z, LEVELS), ((0, 4), (1, 8), (2, 4)), -0.2, 0.2), 0.5, 2.0)
    return {"tracer": tracer, "crowding": crowding}


def inner_cells(values, dims):
    for dim in dims:
        values = lax.slice_in_dim(values, 1, values.shape[dim] - 1, axis=dim)
    return values


def side_cells(values, dim, start, dims):
    others = [other for other in dims if other != dim]
    values = inner_cells(values, others)
    return lax.slice_in_dim(values, start, start + values.shape[dim] - 2, axis=dim)


def advance(padded, crowding):
    middle = inner_cells(padded, (0, 1, 2))
    lower = [side_cells(padded, dim, 0, (0, 1, 2)) for dim in (0, 1, 2)]
    upper = [side_cells(padded, dim, 2, (0, 1, 2)) for dim in (0, 1, 2)]
    spread = lower[0] + upper[0] + lower[1] + upper[1] + lower[2] + upper[2] - 6.0 * middle
    return middle + 0.1 * spread + 0.2 * middle * (1.0 - middle * crowding)


def reference(tracer, crowding):
    for step in range(STEPS):
        tracer = advance(jnp.pad(tracer, ((1, 1), (1, 1), (1, 1), (0, 0)), mode="constant"), crowding)
    column_sum = jnp.cumsum(tracer, axis=0) / GRID_Y
    return column_sum, tracer
```

```python
import functools

import jax
import jax.numpy as jnp
from jax import lax
from jax.experimental import pallas as pl
from jax.experimental.pallas import tpu as pltpu
from jax.sharding import PartitionSpec as P

STEPS = 4
CHUNKS = 8
MESH = pl.DeviceIdType.MESH


def kernel(sizes, tr, cr, out_c, out_t, other, ylo, yhi, xlo, xhi, zlo, zhi, zsl, zsh, q, g,
           load_sem, yu_s, yu_r, yd_s, yd_r, xs, xr, zs, zr, qs, qr):
    rows, cols, slabs = sizes
    ny, nx, nz, nl = tr.shape
    width = nx // CHUNKS
    row, col, slab = (lax.axis_index(a) for a in ("rows", "cols", "slabs"))
    has_up, has_dn = row < rows - 1, row > 0
    has_xu, has_xd = col < cols - 1, col > 0
    has_zu, has_zd = slab < slabs - 1, slab > 0
    fields = (out_t, other)
    first = lax.broadcasted_iota(jnp.int32, (nz, nl), 0) == 0
    final = lax.broadcasted_iota(jnp.int32, (nz, nl), 0) == nz - 1
    inner = jnp.where(has_dn, jnp.float32(0.1), jnp.float32(0.0))

    def chunk(k):
        return pl.ds(pl.multiple_of(k * width, width), width)

    def remote(src, dst, send, recv, axis, index):
        return pltpu.make_async_remote_copy(
            src_ref=src, dst_ref=dst, send_sem=send, recv_sem=recv,
            device_id={axis: index}, device_id_type=MESH)

    up, dn = jnp.minimum(row + 1, rows - 1), jnp.maximum(row - 1, 0)
    xu, xd = jnp.minimum(col + 1, cols - 1), jnp.maximum(col - 1, 0)
    zu, zd = jnp.minimum(slab + 1, slabs - 1), jnp.maximum(slab - 1, 0)

    def y_up(n, k):
        src = tr if n == 0 else fields[n % 2]
        return remote(src.at[ny - 1, chunk(k)], ylo.at[n % 2, chunk(k)], yu_s.at[n, k], yu_r.at[n, k], "rows", up)

    def y_dn(n, k):
        src = tr if n == 0 else fields[n % 2]
        return remote(src.at[0, chunk(k)], yhi.at[n % 2, chunk(k)], yd_s.at[n, k], yd_r.at[n, k], "rows", dn)

    def x_up(n):
        return remote(fields[n % 2].at[:, nx - 1], xlo.at[n % 2], xs.at[n, 0], xr.at[n, 0], "cols", xu)

    def x_dn(n):
        return remote(fields[n % 2].at[:, 0], xhi.at[n % 2], xs.at[n, 1], xr.at[n, 1], "cols", xd)

    def z_up(n):
        return remote(zsh.at[n % 2], zlo.at[n % 2], zs.at[n, 0], zr.at[n, 0], "slabs", zu)

    def z_dn(n):
        return remote(zsl.at[n % 2], zhi.at[n % 2], zs.at[n, 1], zr.at[n, 1], "slabs", zd)

    def q_up(k):
        return remote(g.at[chunk(k)], q.at[chunk(k)], qs.at[k], qr.at[k], "rows", up)

    sides = ((has_xu, has_xd, x_up), (has_xd, has_xu, x_dn), (has_zu, has_zd, z_up), (has_zd, has_zu, z_dn))

    def start_sides(n):
        for sends, _, copy in sides:
            @pl.when(sends)
            def _():
                copy(n).start()

    def wait_side_sends(n):
        for sends, _, copy in sides:
            @pl.when(sends)
            def _():
                copy(n).wait_send()

    def wait_side_recvs(n):
        for _, gets, copy in sides:
            @pl.when(gets)
            def _():
                copy(n).wait_recv()

    def wait_y_sends(n, k):
        @pl.when(has_up)
        def _():
            y_up(n, k).wait_send()

        @pl.when(has_dn)
        def _():
            y_dn(n, k).wait_send()

    def wait_y_recvs(n, k):
        @pl.when(has_dn)
        def _():
            y_up(n, k).wait_recv()

        @pl.when(has_up)
        def _():
            y_dn(n, k).wait_recv()

    def each(count, body, start=0):
        def turn(i, carry):
            body(i)
            return carry
        lax.fori_loop(start, count, turn, 0)

    load_t = pltpu.make_async_copy(tr, out_t, load_sem.at[0])
    load_c = pltpu.make_async_copy(cr, out_c, load_sem.at[1])
    load_t.start()
    load_c.start()

    barrier = pltpu.get_barrier_semaphore()
    count = jnp.int32(0)
    for there, axis, index in ((has_up, "rows", up), (has_dn, "rows", dn), (has_xu, "cols", xu),
                               (has_xd, "cols", xd), (has_zu, "slabs", zu), (has_zd, "slabs", zd)):
        @pl.when(there)
        def _():
            pl.semaphore_signal(barrier, inc=1, device_id={axis: index}, device_id_type=MESH)
        count = count + there.astype(jnp.int32)
    pl.semaphore_wait(barrier, count)

    @pl.when(has_up)
    def _():
        each(CHUNKS, lambda k: y_up(0, k).start())

    @pl.when(has_dn)
    def _():
        each(CHUNKS, lambda k: y_dn(0, k).start())

    zeros = jnp.zeros((nz, nl), jnp.float32)

    @pl.when(jnp.logical_not(has_dn))
    def _():
        def clear(x):
            ylo[0, x] = zeros
            ylo[1, x] = zeros
            q[x] = zeros
        each(nx, clear)

    @pl.when(jnp.logical_not(has_up))
    def _():
        def clear(x):
            yhi[0, x] = zeros
            yhi[1, x] = zeros
        each(nx, clear)

    for there, ref in ((has_xd, xlo), (has_xu, xhi), (has_zd, zlo), (has_zu, zhi)):
        @pl.when(jnp.logical_not(there))
        def _():
            ref[...] = jnp.zeros_like(ref)

    load_t.wait()

    def stage(x):
        for y in range(ny):
            zsl[0, y, pl.ds(x, 1), :] = out_t[y, x, 0:1, :]
            zsh[0, y, pl.ds(x, 1), :] = out_t[y, x, nz - 1:nz, :]
    each(nx, stage)
    start_sides(0)
    load_c.wait()

    def update(n, x, y, left, right, values, low, high):
        now = n % 2
        v = values[y]
        total = left + right
        lower = jnp.where(first, zlo[now, y, pl.ds(x, 1), :], pltpu.roll(v, 1, 0))
        upper = jnp.where(final, zhi[now, y, pl.ds(x, 1), :], pltpu.roll(v, nz - 1, 0))
        total = total + (lower + upper)
        for other_y in (low, high):
            if other_y is not None:
                total = total + other_y
        return v * (0.6 - 0.2 * (out_c[y, x] * v)) + 0.1 * total

    def over_rows(k, body, n):
        src = fields[n % 2]
        now = n % 2
        low = jnp.maximum(k * width, 1)
        high = jnp.minimum((k + 1) * width, nx - 1)

        @pl.when(k == 0)
        def _():
            body(0, lambda y: xlo[now, y], lambda y: src[y, 1])

        each(high, lambda x: body(x, lambda y: src[y, x - 1], lambda y: src[y, x + 1]), low)

        @pl.when(k == CHUNKS - 1)
        def _():
            body(nx - 1, lambda y: src[y, nx - 2], lambda y: xhi[now, y])

    held_from = jnp.minimum(CHUNKS // 2 + 2 * row, CHUNKS)

    for n in range(STEPS - 1):
        src, dst = fields[n % 2], fields[(n + 1) % 2]
        now, later = n % 2, (n + 1) % 2
        if n >= 1:
            wait_side_sends(n - 1)
        wait_side_recvs(n)

        def one_row(x, left, right, n=n, src=src, dst=dst, now=now, later=later):
            values = [src[y, x] for y in range(ny)]
            for y in range(ny):
                below = values[y - 1] if y > 0 else ylo[now, x]
                above = values[y + 1] if y < ny - 1 else yhi[now, x]
                new = update(n, x, y, left(y), right(y), values, below, above)
                dst[y, x] = new
                zsl[later, y, pl.ds(x, 1), :] = new[0:1]
                zsh[later, y, pl.ds(x, 1), :] = new[nz - 1:nz]

        def one_chunk(k, n=n, one_row=one_row):
            wait_y_recvs(n, k)
            if n >= 1:
                wait_y_sends(n - 1, k)
            over_rows(k, one_row, n)
            goes_up = has_up if n + 1 < STEPS - 1 else jnp.logical_and(has_up, k < held_from)

            @pl.when(goes_up)
            def _():
                y_up(n + 1, k).start()

            @pl.when(has_dn)
            def _():
                y_dn(n + 1, k).start()

        each(CHUNKS, one_chunk)
        start_sides(n + 1)

    n = STEPS - 1
    src, dst = fields[n % 2], fields[(n + 1) % 2]
    wait_side_sends(n - 1)
    wait_side_recvs(n)

    def part_row(x, left, right):
        values = [src[y, x] for y in range(ny)]
        total = 0.1 * values[ny - 1] + inner * values[0]
        for y in range(ny):
            below = values[y - 1] if y > 0 else None
            above = values[y + 1] if y < ny - 1 else None
            new = update(n, x, y, left(y), right(y), values, below, above)
            dst[y, x] = new
            total = total + new
        g[x] = total

    def part_chunk(k):
        wait_y_sends(n - 1, k)
        over_rows(k, part_row, n)

        @pl.when(jnp.logical_not(has_dn))
        def _():
            q_up(k).start()
    each(CHUNKS, part_chunk)

    @pl.when(has_dn)
    def _():
        def pass_on(k):
            q_up(k).wait_recv()

            @pl.when(has_up)
            def _():
                def add(x):
                    g[x] = g[x] + q[x]
                each((k + 1) * width, add, k * width)
                q_up(k).start()
        each(CHUNKS, pass_on)

    @pl.when(has_up)
    def _():
        each(CHUNKS, lambda k: y_up(n, k).start(), held_from)

    scale = 1.0 / (ny * rows)

    def end_chunk(k):
        wait_y_recvs(n, k)

        def end_row(x):
            low = ylo[n % 2, x]
            sums = q[x] + inner * (src[0, x] - low)
            for y in range(ny):
                value = dst[y, x]
                if y == 0:
                    value = value + 0.1 * low
                if y == ny - 1:
                    value = value + 0.1 * yhi[n % 2, x]
                if y in (0, ny - 1):
                    dst[y, x] = value
                sums = sums + value
                out_c[y, x] = sums * scale
        each((k + 1) * width, end_row, k * width)
    each(CHUNKS, end_chunk)

    each(CHUNKS, lambda k: wait_y_sends(n, k))
    wait_side_sends(n)

    @pl.when(has_up)
    def _():
        each(CHUNKS, lambda k: q_up(k).wait_send())


def body(tracer, crowding):
    ny, nx, nz, nl = tracer.shape
    sizes = tuple(lax.axis_size(a) for a in ("rows", "cols", "slabs"))
    shape = jax.ShapeDtypeStruct(tracer.shape, jnp.float32)
    vmem = lambda *s: pltpu.VMEM(s, jnp.float32)
    dma = pltpu.SemaphoreType.DMA
    return pl.pallas_call(
        functools.partial(kernel, sizes),
        out_shape=(shape, shape),
        in_specs=[pl.BlockSpec(memory_space=pltpu.HBM)] * 2,
        out_specs=[pl.BlockSpec(memory_space=pltpu.VMEM)] * 2,
        scratch_shapes=[
            vmem(ny, nx, nz, nl),
            vmem(2, nx, nz, nl), vmem(2, nx, nz, nl),
            vmem(2, ny, nz, nl), vmem(2, ny, nz, nl),
            vmem(2, ny, nx, nl), vmem(2, ny, nx, nl),
            vmem(2, ny, nx, nl), vmem(2, ny, nx, nl),
            vmem(nx, nz, nl), vmem(nx, nz, nl),
            dma((2,)),
            dma((STEPS, CHUNKS)), dma((STEPS, CHUNKS)), dma((STEPS, CHUNKS)), dma((STEPS, CHUNKS)),
            dma((STEPS, 2)), dma((STEPS, 2)), dma((STEPS, 2)), dma((STEPS, 2)),
            dma((CHUNKS,)), dma((CHUNKS,)),
        ],
        compiler_params=pltpu.CompilerParams(
            collective_id=0, has_side_effects=True, vmem_limit_bytes=42 * 1024 * 1024),
        name="grid_steps",
    )(tracer, crowding)


def solution(mesh):
    placed = P("rows", "cols", "slabs", None)
    return jax.shard_map(body, mesh=mesh, in_specs=(placed, placed), out_specs=(placed, placed), check_vma=False)
```

```python
import functools

import jax
import jax.numpy as jnp
from jax import lax
from jax.experimental import pallas as pl
from jax.experimental.pallas import tpu as pltpu
from jax.sharding import PartitionSpec as P

STEPS = 4
CHUNKS = 8
PARTS = 16
CUTS = (0, 5, 10, 16)
MESH = pl.DeviceIdType.MESH


def kernel(sizes, tr, cr, out_c, out_t, other, ylo, yhi, xlo, xhi, zlo, zhi, zsl, zsh, qu, qd, g,
           load_sem, yu_s, yu_r, yd_s, yd_r, xs, xr, zs, zr, qu_s, qu_r, qd_s, qd_r):
    rows, cols, slabs = sizes
    ny, nx, nz, nl = tr.shape
    width = nx // CHUNKS
    row, col, slab = (lax.axis_index(a) for a in ("rows", "cols", "slabs"))
    has_up, has_dn = row < rows - 1, row > 0
    has_xu, has_xd = col < cols - 1, col > 0
    has_zu, has_zd = slab < slabs - 1, slab > 0
    fields = (out_t, other)
    first = lax.broadcasted_iota(jnp.int32, (nz, nl), 0) == 0
    final = lax.broadcasted_iota(jnp.int32, (nz, nl), 0) == nz - 1
    inner = jnp.where(has_dn, jnp.float32(0.1), jnp.float32(0.0))

    def chunk(k):
        return pl.ds(pl.multiple_of(k * width, width), width)

    def remote(src, dst, send, recv, axis, index):
        return pltpu.make_async_remote_copy(
            src_ref=src, dst_ref=dst, send_sem=send, recv_sem=recv,
            device_id={axis: index}, device_id_type=MESH)

    up, dn, back = jnp.minimum(row + 1, rows - 1), jnp.maximum(row - 1, 0), lax.rem(row + rows - 1, rows)
    piece = nx // PARTS
    xu, xd = jnp.minimum(col + 1, cols - 1), jnp.maximum(col - 1, 0)
    zu, zd = jnp.minimum(slab + 1, slabs - 1), jnp.maximum(slab - 1, 0)

    def y_up(n, k):
        src = tr if n == 0 else fields[n % 2]
        return remote(src.at[ny - 1, chunk(k)], ylo.at[n % 2, chunk(k)], yu_s.at[n, k], yu_r.at[n, k], "rows", up)

    def y_dn(n, k):
        src = tr if n == 0 else fields[n % 2]
        return remote(src.at[0, chunk(k)], yhi.at[n % 2, chunk(k)], yd_s.at[n, k], yd_r.at[n, k], "rows", dn)

    def x_up(n):
        return remote(fields[n % 2].at[:, nx - 1], xlo.at[n % 2], xs.at[n, 0], xr.at[n, 0], "cols", xu)

    def x_dn(n):
        return remote(fields[n % 2].at[:, 0], xhi.at[n % 2], xs.at[n, 1], xr.at[n, 1], "cols", xd)

    def z_up(n):
        return remote(zsh.at[n % 2], zlo.at[n % 2], zs.at[n, 0], zr.at[n, 0], "slabs", zu)

    def z_dn(n):
        return remote(zsl.at[n % 2], zhi.at[n % 2], zs.at[n, 1], zr.at[n, 1], "slabs", zd)

    def part(j):
        return pl.ds(pl.multiple_of(j * piece, piece), piece)

    def q_up(j):
        return remote(g.at[part(j)], qu.at[part(j)], qu_s.at[j], qu_r.at[j], "rows", up)

    def q_dn(j, src=g):
        return remote(src.at[part(j)], qd.at[part(j)], qd_s.at[j], qd_r.at[j], "rows", back)

    sides = ((has_xu, has_xd, x_up), (has_xd, has_xu, x_dn), (has_zu, has_zd, z_up), (has_zd, has_zu, z_dn))

    def start_sides(n):
        for sends, _, copy in sides:
            @pl.when(sends)
            def _():
                copy(n).start()

    def wait_side_sends(n):
        for sends, _, copy in sides:
            @pl.when(sends)
            def _():
                copy(n).wait_send()

    def wait_side_recvs(n):
        for _, gets, copy in sides:
            @pl.when(gets)
            def _():
                copy(n).wait_recv()

    def wait_y_sends(n, k):
        @pl.when(has_up)
        def _():
            y_up(n, k).wait_send()

        @pl.when(has_dn)
        def _():
            y_dn(n, k).wait_send()

    def wait_y_recvs(n, k):
        @pl.when(has_dn)
        def _():
            y_up(n, k).wait_recv()

        @pl.when(has_up)
        def _():
            y_dn(n, k).wait_recv()

    def each(count, body, start=0):
        def turn(i, carry):
            body(i)
            return carry
        lax.fori_loop(start, count, turn, 0)

    load_t = pltpu.make_async_copy(tr, out_t, load_sem.at[0])
    load_c = pltpu.make_async_copy(cr, out_c, load_sem.at[1])
    load_t.start()
    load_c.start()

    barrier = pltpu.get_barrier_semaphore()
    count = jnp.int32(0)
    for there, axis, index in ((has_up, "rows", up), (has_dn, "rows", dn), (has_xu, "cols", xu),
                               (has_xd, "cols", xd), (has_zu, "slabs", zu), (has_zd, "slabs", zd)):
        @pl.when(there)
        def _():
            pl.semaphore_signal(barrier, inc=1, device_id={axis: index}, device_id_type=MESH)
        count = count + there.astype(jnp.int32)
    ends = jnp.logical_or(row == 0, row == rows - 1)

    @pl.when(ends)
    def _():
        pl.semaphore_signal(barrier, inc=1, device_id={"rows": rows - 1 - row}, device_id_type=MESH)
    pl.semaphore_wait(barrier, count + ends.astype(jnp.int32))

    @pl.when(has_up)
    def _():
        each(CHUNKS, lambda k: y_up(0, k).start())

    @pl.when(has_dn)
    def _():
        each(CHUNKS, lambda k: y_dn(0, k).start())

    zeros = jnp.zeros((nz, nl), jnp.float32)

    @pl.when(jnp.logical_not(has_dn))
    def _():
        def clear(x):
            ylo[0, x] = zeros
            ylo[1, x] = zeros
        each(nx, clear)

    @pl.when(jnp.logical_not(has_up))
    def _():
        def clear(x):
            yhi[0, x] = zeros
            yhi[1, x] = zeros
        each(nx, clear)

    for there, ref in ((has_xd, xlo), (has_xu, xhi), (has_zd, zlo), (has_zu, zhi)):
        @pl.when(jnp.logical_not(there))
        def _():
            ref[...] = jnp.zeros_like(ref)

    load_t.wait()

    def stage(x):
        for y in range(ny):
            zsl[0, y, pl.ds(x, 1), :] = out_t[y, x, 0:1, :]
            zsh[0, y, pl.ds(x, 1), :] = out_t[y, x, nz - 1:nz, :]
    each(nx, stage)
    start_sides(0)
    load_c.wait()

    def update(n, x, y, left, right, values, low, high):
        now = n % 2
        v = values[y]
        total = left + right
        lower = jnp.where(first, zlo[now, y, pl.ds(x, 1), :], pltpu.roll(v, 1, 0))
        upper = jnp.where(final, zhi[now, y, pl.ds(x, 1), :], pltpu.roll(v, nz - 1, 0))
        total = total + (lower + upper)
        for other_y in (low, high):
            if other_y is not None:
                total = total + other_y
        return v * (0.6 - 0.2 * (out_c[y, x] * v)) + 0.1 * total

    def over_rows(k, body, n):
        src = fields[n % 2]
        now = n % 2
        low = jnp.maximum(k * width, 1)
        high = jnp.minimum((k + 1) * width, nx - 1)

        @pl.when(k == 0)
        def _():
            body(0, lambda y: xlo[now, y], lambda y: src[y, 1])

        each(high, lambda x: body(x, lambda y: src[y, x - 1], lambda y: src[y, x + 1]), low)

        @pl.when(k == CHUNKS - 1)
        def _():
            body(nx - 1, lambda y: src[y, nx - 2], lambda y: xhi[now, y])

    held_from = CHUNKS // 2

    for n in range(STEPS - 1):
        src, dst = fields[n % 2], fields[(n + 1) % 2]
        now, later = n % 2, (n + 1) % 2
        if n >= 1:
            wait_side_sends(n - 1)
        wait_side_recvs(n)

        def one_row(x, left, right, n=n, src=src, dst=dst, now=now, later=later):
            values = [src[y, x] for y in range(ny)]
            for y in range(ny):
                below = values[y - 1] if y > 0 else ylo[now, x]
                above = values[y + 1] if y < ny - 1 else yhi[now, x]
                new = update(n, x, y, left(y), right(y), values, below, above)
                dst[y, x] = new
                zsl[later, y, pl.ds(x, 1), :] = new[0:1]
                zsh[later, y, pl.ds(x, 1), :] = new[nz - 1:nz]

        def one_chunk(k, n=n, one_row=one_row):
            wait_y_recvs(n, k)
            if n >= 1:
                wait_y_sends(n - 1, k)
            over_rows(k, one_row, n)
            goes_up = has_up if n + 1 < STEPS - 1 else jnp.logical_and(has_up, k < held_from)

            @pl.when(goes_up)
            def _():
                y_up(n + 1, k).start()

            goes_dn = has_dn if n + 1 < STEPS - 1 else jnp.logical_and(has_dn, k < held_from)

            @pl.when(goes_dn)
            def _():
                y_dn(n + 1, k).start()

        each(CHUNKS, one_chunk)
        start_sides(n + 1)

    n = STEPS - 1
    src, dst = fields[n % 2], fields[(n + 1) % 2]
    wait_side_sends(n - 1)
    wait_side_recvs(n)

    def part_row(x, left, right):
        values = [src[y, x] for y in range(ny)]
        total = 0.1 * values[ny - 1] + inner * values[0]
        for y in range(ny):
            below = values[y - 1] if y > 0 else None
            above = values[y + 1] if y < ny - 1 else None
            new = update(n, x, y, left(y), right(y), values, below, above)
            dst[y, x] = new
            total = total + new
        g[x] = total

    def part_chunk(k):
        wait_y_sends(n - 1, k)
        over_rows(k, part_row, n)
    each(CHUNKS, part_chunk)

    def parts(s, body):
        each(CUTS[s + 1], body, CUTS[s])

    def over(j, body):
        each((j + 1) * piece, body, j * piece)

    def send(copy):
        return lambda j: copy(j).start()

    def rest_up():
        each(CHUNKS, lambda k: y_up(n, k).start(), held_from)

    def rest_dn():
        each(CHUNKS, lambda k: y_dn(n, k).start(), held_from)

    @pl.when(row == 0)
    def _():
        parts(0, send(q_dn))
        parts(2, send(q_up))
        parts(1, send(q_up))
        rest_up()

        def around(j):
            q_dn(j).wait_recv()

            def add(x):
                qd[x] = qd[x] + g[x]
            over(j, add)
            q_dn(j, qd).start()
        parts(1, around)
        parts(2, around)

    @pl.when(row == 1)
    def _():
        parts(1, send(q_dn))
        parts(0, send(q_up))

        def both(j):
            q_up(j).wait_recv()
            q_dn(j).wait_recv()

            def add(x):
                own = g[x]
                qd[x] = qd[x] + own
                g[x] = qu[x] + own
            over(j, add)
            q_up(j).start()
            q_dn(j, qd).start()
        parts(2, both)
        rest_up()
        rest_dn()
        each(CUTS[2], lambda j: q_up(j).wait_recv(), CUTS[1])
        each(CUTS[1], lambda j: q_dn(j).wait_recv(), CUTS[0])

    @pl.when(row == 2)
    def _():
        parts(2, send(q_dn))
        parts(1, send(q_up))

        def both(j):
            q_up(j).wait_recv()

            def add(x):
                g[x] = qu[x] + g[x]
            over(j, add)
            q_up(j).start()
            q_dn(j).wait_recv()
            q_dn(j, qd).start()
        parts(0, both)
        rest_up()
        rest_dn()
        parts(1, lambda j: q_dn(j).wait_recv())
        parts(2, lambda j: q_up(j).wait_recv())

    @pl.when(row == 3)
    def _():
        def forward(j):
            q_dn(j).wait_recv()
            q_dn(j, qd).start()
        parts(0, forward)
        parts(1, forward)
        rest_dn()
        parts(0, lambda j: q_up(j).wait_recv())
        parts(1, lambda j: q_up(j).wait_recv())
        parts(2, lambda j: q_dn(j).wait_recv())

    scale = 1.0 / (ny * rows)

    def end_chunk(k):
        wait_y_recvs(n, k)

        def end_row(x):
            low = ylo[n % 2, x]
            kind = (x >= CUTS[1] * piece).astype(jnp.int32) + (x >= CUTS[2] * piece).astype(jnp.int32)
            use_u = jnp.logical_and(has_dn, kind != row - 1)
            use_d = jnp.logical_and(has_dn, kind <= row - 1)
            sums = lax.select(use_u, qu[x], zeros) + lax.select(use_d, qd[x], zeros)
            sums = sums + inner * (src[0, x] - low)
            for y in range(ny):
                value = dst[y, x]
                if y == 0:
                    value = value + 0.1 * low
                if y == ny - 1:
                    value = value + 0.1 * yhi[n % 2, x]
                if y in (0, ny - 1):
                    dst[y, x] = value
                sums = sums + value
                out_c[y, x] = sums * scale
        each((k + 1) * width, end_row, k * width)
    each(CHUNKS, end_chunk)

    each(CHUNKS, lambda k: wait_y_sends(n, k))
    wait_side_sends(n)

    for r in range(rows):
        @pl.when(row == r)
        def _():
            for kind in range(3):
                if r < rows - 1 and kind != r:
                    parts(kind, lambda j: q_up(j).wait_send())
                if kind not in {0: (), 1: (0,), 2: (1,), 3: (2,)}[r]:
                    parts(kind, lambda j: q_dn(j).wait_send())


def write(c_ref, t_ref, out_c, out_t, sem):
    copies = [pltpu.make_async_copy(c_ref, out_c, sem.at[0]), pltpu.make_async_copy(t_ref, out_t, sem.at[1])]
    for copy in copies:
        copy.start()
    for copy in copies:
        copy.wait()


def body(tracer, crowding):
    ny, nx, nz, nl = tracer.shape
    sizes = tuple(lax.axis_size(a) for a in ("rows", "cols", "slabs"))
    shape = jax.ShapeDtypeStruct(tracer.shape, jnp.float32)
    vmem = lambda *s: pltpu.VMEM(s, jnp.float32)
    dma = pltpu.SemaphoreType.DMA
    sums, field = pl.pallas_call(
        functools.partial(kernel, sizes),
        out_shape=(shape, shape),
        in_specs=[pl.BlockSpec(memory_space=pltpu.HBM)] * 2,
        out_specs=[pl.BlockSpec(memory_space=pltpu.VMEM)] * 2,
        scratch_shapes=[
            vmem(ny, nx, nz, nl),
            vmem(2, nx, nz, nl), vmem(2, nx, nz, nl),
            vmem(2, ny, nz, nl), vmem(2, ny, nz, nl),
            vmem(2, ny, nx, nl), vmem(2, ny, nx, nl),
            vmem(2, ny, nx, nl), vmem(2, ny, nx, nl),
            vmem(nx, nz, nl), vmem(nx, nz, nl), vmem(nx, nz, nl),
            dma((2,)),
            dma((STEPS, CHUNKS)), dma((STEPS, CHUNKS)), dma((STEPS, CHUNKS)), dma((STEPS, CHUNKS)),
            dma((STEPS, 2)), dma((STEPS, 2)), dma((STEPS, 2)), dma((STEPS, 2)),
            dma((PARTS,)), dma((PARTS,)), dma((PARTS,)), dma((PARTS,)),
        ],
        compiler_params=pltpu.CompilerParams(
            collective_id=0, has_side_effects=True, vmem_limit_bytes=30 * 1024 * 1024),
        name="grid_steps",
    )(tracer, crowding)
    return pl.pallas_call(
        write,
        out_shape=(shape, shape),
        in_specs=[pl.BlockSpec(memory_space=pltpu.VMEM)] * 2,
        out_specs=[pl.BlockSpec(memory_space=pltpu.HBM)] * 2,
        scratch_shapes=[dma((2,))],
        compiler_params=pltpu.CompilerParams(vmem_limit_bytes=1024 * 1024),
        name="write_out",
    )(sums, field)


def solution(mesh):
    placed = P("rows", "cols", "slabs", None)
    return jax.shard_map(body, mesh=mesh, in_specs=(placed, placed), out_specs=(placed, placed), check_vma=False)
```

```python
import functools

import jax
import jax.numpy as jnp
from jax import lax
from jax.experimental import pallas as pl
from jax.experimental.pallas import tpu as pltpu
from jax.sharding import PartitionSpec as P

STEPS = 4
CHUNKS = 4
HELD = 3
WRITES = 4
SHARES = (22, 21, 21)
MESH = pl.DeviceIdType.MESH


def column_sets(nx):
    counts = [share * nx // sum(SHARES) for share in SHARES]
    counts[2] = nx - counts[0] - counts[1]
    sets, start, base = [], 0, 0
    for count in counts:
        piece = next(p for p in (11, 7, 6, 5, 4, 3, 2, 1) if count % p == 0)
        sets.append((start, count // piece, piece, base))
        start, base = start + count, base + count // piece
    return sets


def kernel(sizes, tr, cr, out_c, out_t, other, ylo, yhi, xlo, xhi, zlo, zhi, zsl, zsh, qu, qd, g,
           load_sem, yu_s, yu_r, yd_s, yd_r, xs, xr, zs, zr, qu_s, qu_r, qd_s, qd_r):
    rows, cols, slabs = sizes
    ny, nx, nz, nl = tr.shape
    width = nx // CHUNKS
    row, col, slab = (lax.axis_index(a) for a in ("rows", "cols", "slabs"))
    has_up, has_dn = row < rows - 1, row > 0
    has_xu, has_xd = col < cols - 1, col > 0
    has_zu, has_zd = slab < slabs - 1, slab > 0
    fields = (out_t, other)
    first = lax.broadcasted_iota(jnp.int32, (nz, nl), 0) == 0
    final = lax.broadcasted_iota(jnp.int32, (nz, nl), 0) == nz - 1
    inner = jnp.where(has_dn, jnp.float32(0.1), jnp.float32(0.0))

    def chunk(k):
        return pl.ds(pl.multiple_of(k * width, width), width)

    def remote(src, dst, send, recv, axis, index):
        return pltpu.make_async_remote_copy(
            src_ref=src, dst_ref=dst, send_sem=send, recv_sem=recv,
            device_id={axis: index}, device_id_type=MESH)

    up, dn, back = jnp.minimum(row + 1, rows - 1), jnp.maximum(row - 1, 0), lax.rem(row + rows - 1, rows)
    sets = column_sets(nx)
    xu, xd = jnp.minimum(col + 1, cols - 1), jnp.maximum(col - 1, 0)
    zu, zd = jnp.minimum(slab + 1, slabs - 1), jnp.maximum(slab - 1, 0)

    def y_up(n, k):
        return remote(fields[n % 2].at[ny - 1, chunk(k)], ylo.at[n % 2, chunk(k)], yu_s.at[n, k], yu_r.at[n, k], "rows", up)

    def y_dn(n, k):
        return remote(fields[n % 2].at[0, chunk(k)], yhi.at[n % 2, chunk(k)], yd_s.at[n, k], yd_r.at[n, k], "rows", dn)

    def x_up(n):
        return remote(fields[n % 2].at[:, nx - 1], xlo.at[n % 2], xs.at[n, 0], xr.at[n, 0], "cols", xu)

    def x_dn(n):
        return remote(fields[n % 2].at[:, 0], xhi.at[n % 2], xs.at[n, 1], xr.at[n, 1], "cols", xd)

    def z_up(n):
        return remote(zsh.at[n % 2], zlo.at[n % 2], zs.at[n, 0], zr.at[n, 0], "slabs", zu)

    def z_dn(n):
        return remote(zsl.at[n % 2], zhi.at[n % 2], zs.at[n, 1], zr.at[n, 1], "slabs", zd)

    def part(kind, i):
        start, _, piece, _ = sets[kind]
        return pl.ds(start + i * piece, piece)

    def q_up(kind, i):
        j = sets[kind][3] + i
        return remote(g.at[part(kind, i)], qu.at[part(kind, i)], qu_s.at[j], qu_r.at[j], "rows", up)

    def q_dn(kind, i, src=g):
        j = sets[kind][3] + i
        return remote(src.at[part(kind, i)], qd.at[part(kind, i)], qd_s.at[j], qd_r.at[j], "rows", back)

    sides = ((has_xu, has_xd, x_up), (has_xd, has_xu, x_dn), (has_zu, has_zd, z_up), (has_zd, has_zu, z_dn))

    def start_sides(n):
        for sends, _, copy in sides:
            @pl.when(sends)
            def _():
                copy(n).start()

    def wait_side_sends(n):
        for sends, _, copy in sides:
            @pl.when(sends)
            def _():
                copy(n).wait_send()

    def wait_side_recvs(n):
        for _, gets, copy in sides:
            @pl.when(gets)
            def _():
                copy(n).wait_recv()

    def wait_y_sends(n, k):
        @pl.when(has_up)
        def _():
            y_up(n, k).wait_send()

        @pl.when(has_dn)
        def _():
            y_dn(n, k).wait_send()

    def wait_y_recvs(n, k):
        @pl.when(has_dn)
        def _():
            y_up(n, k).wait_recv()

        @pl.when(has_up)
        def _():
            y_dn(n, k).wait_recv()

    def each(count, body, start=0):
        def turn(i, carry):
            body(i)
            return carry
        lax.fori_loop(start, count, turn, 0)

    inside = pl.ds(1, ny - 2)
    load_ends = [pltpu.make_async_copy(tr.at[y], out_t.at[y], load_sem.at[i]) for i, y in enumerate((0, ny - 1))]
    load_t = pltpu.make_async_copy(tr.at[inside], out_t.at[inside], load_sem.at[2])
    load_c = pltpu.make_async_copy(cr, out_c, load_sem.at[3])
    for load in load_ends:
        load.start()
    load_t.start()
    load_c.start()

    barrier = pltpu.get_barrier_semaphore()
    count = jnp.int32(0)
    for there, axis, index in ((has_up, "rows", up), (has_dn, "rows", dn), (has_xu, "cols", xu),
                               (has_xd, "cols", xd), (has_zu, "slabs", zu), (has_zd, "slabs", zd)):
        @pl.when(there)
        def _():
            pl.semaphore_signal(barrier, inc=1, device_id={axis: index}, device_id_type=MESH)
        count = count + there.astype(jnp.int32)
    ends = jnp.logical_or(row == 0, row == rows - 1)

    @pl.when(ends)
    def _():
        pl.semaphore_signal(barrier, inc=1, device_id={"rows": rows - 1 - row}, device_id_type=MESH)
    pl.semaphore_wait(barrier, count + ends.astype(jnp.int32))

    for load in load_ends:
        load.wait()

    @pl.when(has_up)
    def _():
        each(CHUNKS, lambda k: y_up(0, k).start())

    @pl.when(has_dn)
    def _():
        each(CHUNKS, lambda k: y_dn(0, k).start())

    zeros = jnp.zeros((nz, nl), jnp.float32)

    @pl.when(jnp.logical_not(has_dn))
    def _():
        def clear(x):
            ylo[0, x] = zeros
            ylo[1, x] = zeros
        each(nx, clear)

    @pl.when(jnp.logical_not(has_up))
    def _():
        def clear(x):
            yhi[0, x] = zeros
            yhi[1, x] = zeros
        each(nx, clear)

    for there, ref in ((has_xd, xlo), (has_xu, xhi), (has_zd, zlo), (has_zu, zhi)):
        @pl.when(jnp.logical_not(there))
        def _():
            ref[...] = jnp.zeros_like(ref)

    load_t.wait()

    def stage(x):
        for y in range(ny):
            zsl[0, y, pl.ds(x, 1), :] = out_t[y, x, 0:1, :]
            zsh[0, y, pl.ds(x, 1), :] = out_t[y, x, nz - 1:nz, :]
    each(nx, stage)
    start_sides(0)
    load_c.wait()

    def update(n, x, y, left, right, values, low, high):
        now = n % 2
        v = values[y]
        total = left + right
        lower = jnp.where(first, zlo[now, y, pl.ds(x, 1), :], pltpu.roll(v, 1, 0))
        upper = jnp.where(final, zhi[now, y, pl.ds(x, 1), :], pltpu.roll(v, nz - 1, 0))
        total = total + (lower + upper)
        for other_y in (low, high):
            if other_y is not None:
                total = total + other_y
        return v * (0.6 - 0.2 * (out_c[y, x] * v)) + 0.1 * total

    def over_rows(k, body, n):
        src = fields[n % 2]
        now = n % 2
        low = jnp.maximum(k * width, 1)
        high = jnp.minimum((k + 1) * width, nx - 1)

        @pl.when(k == 0)
        def _():
            body(0, lambda y: xlo[now, y], lambda y: src[y, 1])

        each(high, lambda x: body(x, lambda y: src[y, x - 1], lambda y: src[y, x + 1]), low)

        @pl.when(k == CHUNKS - 1)
        def _():
            body(nx - 1, lambda y: src[y, nx - 2], lambda y: xhi[now, y])

    held_from = HELD

    for n in range(STEPS - 1):
        src, dst = fields[n % 2], fields[(n + 1) % 2]
        now, later = n % 2, (n + 1) % 2
        if n >= 1:
            wait_side_sends(n - 1)
        wait_side_recvs(n)

        def one_row(x, left, right, n=n, src=src, dst=dst, now=now, later=later):
            values = [src[y, x] for y in range(ny)]
            for y in range(ny):
                below = values[y - 1] if y > 0 else ylo[now, x]
                above = values[y + 1] if y < ny - 1 else yhi[now, x]
                new = update(n, x, y, left(y), right(y), values, below, above)
                dst[y, x] = new
                zsl[later, y, pl.ds(x, 1), :] = new[0:1]
                zsh[later, y, pl.ds(x, 1), :] = new[nz - 1:nz]

        def one_chunk(k, n=n, one_row=one_row):
            wait_y_recvs(n, k)
            if n >= 1:
                wait_y_sends(n - 1, k)
            over_rows(k, one_row, n)
            goes_up = has_up if n + 1 < STEPS - 1 else jnp.logical_and(has_up, k < held_from)

            @pl.when(goes_up)
            def _():
                y_up(n + 1, k).start()

            goes_dn = has_dn if n + 1 < STEPS - 1 else jnp.logical_and(has_dn, k < held_from)

            @pl.when(goes_dn)
            def _():
                y_dn(n + 1, k).start()

        each(CHUNKS, one_chunk)
        start_sides(n + 1)

    n = STEPS - 1
    src, dst = fields[n % 2], fields[(n + 1) % 2]
    wait_side_sends(n - 1)
    wait_side_recvs(n)

    def part_row(x, left, right):
        values = [src[y, x] for y in range(ny)]
        total = 0.1 * values[ny - 1] + inner * values[0]
        for y in range(ny):
            below = values[y - 1] if y > 0 else None
            above = values[y + 1] if y < ny - 1 else None
            new = update(n, x, y, left(y), right(y), values, below, above)
            dst[y, x] = new
            total = total + new
        g[x] = total

    def part_chunk(k):
        wait_y_sends(n - 1, k)
        over_rows(k, part_row, n)
    each(CHUNKS, part_chunk)

    def parts(kind, body):
        each(sets[kind][1], lambda i: body(kind, i))

    def over(kind, i, body):
        start, _, piece, _ = sets[kind]
        each(start + (i + 1) * piece, body, start + i * piece)

    def send(copy):
        return lambda kind, i: copy(kind, i).start()

    def rest_up():
        each(CHUNKS, lambda k: y_up(n, k).start(), held_from)

    def rest_dn():
        each(CHUNKS, lambda k: y_dn(n, k).start(), held_from)

    @pl.when(row == 0)
    def _():
        parts(0, send(q_dn))
        parts(2, send(q_up))
        parts(1, send(q_up))
        rest_up()

        def around(kind, i):
            q_dn(kind, i).wait_recv()

            def add(x):
                qd[x] = qd[x] + g[x]
            over(kind, i, add)
            q_dn(kind, i, qd).start()
        parts(1, around)
        parts(2, around)

    @pl.when(row == 1)
    def _():
        parts(1, send(q_dn))
        parts(0, send(q_up))

        def both(kind, i):
            q_up(kind, i).wait_recv()
            q_dn(kind, i).wait_recv()

            def add(x):
                own = g[x]
                qd[x] = qd[x] + own
                g[x] = qu[x] + own
            over(kind, i, add)
            q_up(kind, i).start()
            q_dn(kind, i, qd).start()
        parts(2, both)
        rest_up()
        rest_dn()
        parts(1, lambda kind, i: q_up(kind, i).wait_recv())
        parts(0, lambda kind, i: q_dn(kind, i).wait_recv())

    @pl.when(row == 2)
    def _():
        parts(2, send(q_dn))
        parts(1, send(q_up))

        def both(kind, i):
            q_up(kind, i).wait_recv()

            def add(x):
                g[x] = qu[x] + g[x]
            over(kind, i, add)
            q_up(kind, i).start()
            q_dn(kind, i).wait_recv()
            q_dn(kind, i, qd).start()
        parts(0, both)
        rest_up()
        rest_dn()
        parts(1, lambda kind, i: q_dn(kind, i).wait_recv())
        parts(2, lambda kind, i: q_up(kind, i).wait_recv())

    @pl.when(row == 3)
    def _():
        def forward(kind, i):
            q_dn(kind, i).wait_recv()
            q_dn(kind, i, qd).start()
        parts(0, forward)
        parts(1, forward)
        rest_dn()
        parts(0, lambda kind, i: q_up(kind, i).wait_recv())
        parts(1, lambda kind, i: q_up(kind, i).wait_recv())
        parts(2, lambda kind, i: q_dn(kind, i).wait_recv())

    scale = 1.0 / (ny * rows)

    def end_chunk(k):
        wait_y_recvs(n, k)

        def end_row(x):
            low = ylo[n % 2, x]
            kind = (x >= sets[1][0]).astype(jnp.int32) + (x >= sets[2][0]).astype(jnp.int32)
            use_u = jnp.logical_and(has_dn, kind != row - 1)
            use_d = jnp.logical_and(has_dn, kind <= row - 1)
            sums = lax.select(use_u, qu[x], zeros) + lax.select(use_d, qd[x], zeros)
            sums = sums + inner * (src[0, x] - low)
            for y in range(ny):
                value = dst[y, x]
                if y == 0:
                    value = value + 0.1 * low
                if y == ny - 1:
                    value = value + 0.1 * yhi[n % 2, x]
                if y in (0, ny - 1):
                    dst[y, x] = value
                sums = sums + value
                out_c[y, x] = sums * scale
        each((k + 1) * width, end_row, k * width)
    each(CHUNKS, end_chunk)

    each(CHUNKS, lambda k: wait_y_sends(n, k))
    wait_side_sends(n)

    for r in range(rows):
        @pl.when(row == r)
        def _():
            for kind in range(3):
                if r < rows - 1 and kind != r:
                    parts(kind, lambda kind, i: q_up(kind, i).wait_send())
                if kind not in {0: (), 1: (0,), 2: (1,), 3: (2,)}[r]:
                    parts(kind, lambda kind, i: q_dn(kind, i).wait_send())


def write(c_ref, t_ref, out_c, out_t, sem):
    copies = []
    for i, (src, dst) in enumerate(((c_ref, out_c), (t_ref, out_t))):
        for j in range(WRITES):
            width = src.shape[1] // WRITES
            at = (slice(None), pl.ds(j * width, width)) if WRITES > src.shape[0] else (pl.ds(j * (src.shape[0] // WRITES), src.shape[0] // WRITES),)
            copies.append(pltpu.make_async_copy(src.at[at], dst.at[at], sem.at[i, j]))
    for copy in copies:
        copy.start()
    for copy in copies:
        copy.wait()


def body(tracer, crowding):
    ny, nx, nz, nl = tracer.shape
    sizes = tuple(lax.axis_size(a) for a in ("rows", "cols", "slabs"))
    shape = jax.ShapeDtypeStruct(tracer.shape, jnp.float32)
    vmem = lambda *s: pltpu.VMEM(s, jnp.float32)
    dma = pltpu.SemaphoreType.DMA
    parts = sum(count for _, count, _, _ in column_sets(nx))
    sums, field = pl.pallas_call(
        functools.partial(kernel, sizes),
        out_shape=(shape, shape),
        in_specs=[pl.BlockSpec(memory_space=pltpu.HBM)] * 2,
        out_specs=[pl.BlockSpec(memory_space=pltpu.VMEM)] * 2,
        scratch_shapes=[
            vmem(ny, nx, nz, nl),
            vmem(2, nx, nz, nl), vmem(2, nx, nz, nl),
            vmem(2, ny, nz, nl), vmem(2, ny, nz, nl),
            vmem(2, ny, nx, nl), vmem(2, ny, nx, nl),
            vmem(2, ny, nx, nl), vmem(2, ny, nx, nl),
            vmem(nx, nz, nl), vmem(nx, nz, nl), vmem(nx, nz, nl),
            dma((4,)),
            dma((STEPS, CHUNKS)), dma((STEPS, CHUNKS)), dma((STEPS, CHUNKS)), dma((STEPS, CHUNKS)),
            dma((STEPS, 2)), dma((STEPS, 2)), dma((STEPS, 2)), dma((STEPS, 2)),
            dma((parts,)), dma((parts,)), dma((parts,)), dma((parts,)),
        ],
        compiler_params=pltpu.CompilerParams(
            collective_id=0, has_side_effects=True, vmem_limit_bytes=30 * 1024 * 1024),
        name="grid_steps",
    )(tracer, crowding)
    return pl.pallas_call(
        write,
        out_shape=(shape, shape),
        in_specs=[pl.BlockSpec(memory_space=pltpu.VMEM)] * 2,
        out_specs=[pl.BlockSpec(memory_space=pltpu.HBM)] * 2,
        scratch_shapes=[dma((2, WRITES))],
        compiler_params=pltpu.CompilerParams(vmem_limit_bytes=1024 * 1024),
        name="write_out",
    )(sums, field)


def solution(mesh):
    placed = P("rows", "cols", "slabs", None)
    return jax.shard_map(body, mesh=mesh, in_specs=(placed, placed), out_specs=(placed, placed), check_vma=False)
```

```python
import functools

import jax
import jax.numpy as jnp
from jax import lax
from jax.experimental import pallas as pl
from jax.experimental.pallas import tpu as pltpu
from jax.sharding import PartitionSpec as P

STEPS = 4
CHUNKS = 2
HELD = 1
TAILS = 4
WRITES = 4
SHARES = (22, 21, 21)
MESH = pl.DeviceIdType.MESH


def column_sets(nx):
    counts = [share * nx // sum(SHARES) for share in SHARES]
    counts[2] = nx - counts[0] - counts[1]
    sets, start, base = [], 0, 0
    for count in counts:
        piece = next(p for p in (11, 7, 6, 5, 4, 3, 2, 1) if count % p == 0)
        sets.append((start, count // piece, piece, base))
        start, base = start + count, base + count // piece
    return sets


def kernel(sizes, tr, cr, out_c, out_t, other, ylo, yhi, xlo, xhi, zlo, zhi, zsl, zsh, qu, qd, g,
           load_sem, yu_s, yu_r, yd_s, yd_r, xs, xr, zs, zr, qu_s, qu_r, qd_s, qd_r, tail_s, tail_r):
    rows, cols, slabs = sizes
    ny, nx, nz, nl = tr.shape
    width = nx // CHUNKS
    row, col, slab = (lax.axis_index(a) for a in ("rows", "cols", "slabs"))
    has_up, has_dn = row < rows - 1, row > 0
    has_xu, has_xd = col < cols - 1, col > 0
    has_zu, has_zd = slab < slabs - 1, slab > 0
    fields = (out_t, other)
    first = lax.broadcasted_iota(jnp.int32, (nz, nl), 0) == 0
    final = lax.broadcasted_iota(jnp.int32, (nz, nl), 0) == nz - 1
    inner = jnp.where(has_dn, jnp.float32(0.1), jnp.float32(0.0))

    early = slab < slabs // 2
    below_middle, above_middle = col == cols // 2 - 1, col == cols // 2
    late_xu = jnp.logical_and(below_middle, early)
    late_xd = jnp.logical_and(above_middle, jnp.logical_not(early))
    quiet_xu = jnp.logical_and(below_middle, jnp.logical_not(early))
    quiet_xd = jnp.logical_and(above_middle, early)

    def both_but(a, b):
        return jnp.logical_and(a, jnp.logical_not(b))

    def chunk(k):
        return pl.ds(pl.multiple_of(k * width, width), width)

    def remote(src, dst, send, recv, axis, index):
        return pltpu.make_async_remote_copy(
            src_ref=src, dst_ref=dst, send_sem=send, recv_sem=recv,
            device_id={axis: index}, device_id_type=MESH)

    up, dn, back = jnp.minimum(row + 1, rows - 1), jnp.maximum(row - 1, 0), lax.rem(row + rows - 1, rows)
    sets = column_sets(nx)
    xu, xd = jnp.minimum(col + 1, cols - 1), jnp.maximum(col - 1, 0)
    zu, zd = jnp.minimum(slab + 1, slabs - 1), jnp.maximum(slab - 1, 0)

    def y_up(n, k):
        return remote(fields[n % 2].at[ny - 1, chunk(k)], ylo.at[n % 2, chunk(k)], yu_s.at[n, k], yu_r.at[n, k], "rows", up)

    def y_dn(n, k):
        return remote(fields[n % 2].at[0, chunk(k)], yhi.at[n % 2, chunk(k)], yd_s.at[n, k], yd_r.at[n, k], "rows", dn)

    def tail(j):
        start = HELD * width
        size = (nx - start) // TAILS
        return pl.ds(start + j * size, size)

    def tail_up(j):
        here = fields[(STEPS - 1) % 2].at[ny - 1, tail(j)]
        return remote(here, ylo.at[(STEPS - 1) % 2, tail(j)], tail_s.at[0, j], tail_r.at[0, j], "rows", up)

    def tail_dn(j):
        here = fields[(STEPS - 1) % 2].at[0, tail(j)]
        return remote(here, yhi.at[(STEPS - 1) % 2, tail(j)], tail_s.at[1, j], tail_r.at[1, j], "rows", dn)

    def x_up(n):
        return remote(fields[n % 2].at[:, nx - 1], xlo.at[n % 2], xs.at[n, 0], xr.at[n, 0], "cols", xu)

    def x_dn(n):
        return remote(fields[n % 2].at[:, 0], xhi.at[n % 2], xs.at[n, 1], xr.at[n, 1], "cols", xd)

    def z_up(n):
        return remote(zsh.at[n % 2], zlo.at[n % 2], zs.at[n, 0], zr.at[n, 0], "slabs", zu)

    def z_dn(n):
        return remote(zsl.at[n % 2], zhi.at[n % 2], zs.at[n, 1], zr.at[n, 1], "slabs", zd)

    def part(kind, i):
        start, _, piece, _ = sets[kind]
        return pl.ds(start + i * piece, piece)

    def q_up(kind, i):
        j = sets[kind][3] + i
        return remote(g.at[part(kind, i)], qu.at[part(kind, i)], qu_s.at[j], qu_r.at[j], "rows", up)

    def q_dn(kind, i, src=g):
        j = sets[kind][3] + i
        return remote(src.at[part(kind, i)], qd.at[part(kind, i)], qd_s.at[j], qd_r.at[j], "rows", back)

    sides = ((has_xu, has_xd, x_up), (has_xd, has_xu, x_dn), (has_zu, has_zd, z_up), (has_zd, has_zu, z_dn))

    def start_sides(n):
        for sends, _, copy in sides:
            if n == 0 and copy is x_up:
                sends = both_but(sends, late_xu)
            if n == 0 and copy is x_dn:
                sends = both_but(sends, late_xd)

            @pl.when(sends)
            def _():
                copy(n).start()

    def wait_side_sends(n):
        for sends, _, copy in sides:
            @pl.when(sends)
            def _():
                copy(n).wait_send()

    def wait_side_recvs(n):
        for _, gets, copy in sides:
            @pl.when(gets)
            def _():
                copy(n).wait_recv()

    def wait_y_sends(n, k):
        @pl.when(has_up)
        def _():
            y_up(n, k).wait_send()

        @pl.when(has_dn)
        def _():
            y_dn(n, k).wait_send()

    def wait_y_recvs(n, k):
        @pl.when(has_dn)
        def _():
            y_up(n, k).wait_recv()

        @pl.when(has_up)
        def _():
            y_dn(n, k).wait_recv()

    def each(count, body, start=0):
        def turn(i, carry):
            body(i)
            return carry
        lax.fori_loop(start, count, turn, 0)

    inside = pl.ds(1, ny - 2)
    load_ends = [pltpu.make_async_copy(tr.at[y], out_t.at[y], load_sem.at[i]) for i, y in enumerate((0, ny - 1))]
    load_t = pltpu.make_async_copy(tr.at[inside], out_t.at[inside], load_sem.at[2])
    load_c = pltpu.make_async_copy(cr, out_c, load_sem.at[3])
    for load in load_ends:
        load.start()
    load_t.start()
    load_c.start()

    barrier = pltpu.get_barrier_semaphore()
    count = jnp.int32(0)
    for says, hears, axis, index in (
            (has_up, has_up, "rows", up), (has_dn, has_dn, "rows", dn),
            (both_but(has_xu, quiet_xu), both_but(has_xu, late_xu), "cols", xu),
            (both_but(has_xd, quiet_xd), both_but(has_xd, late_xd), "cols", xd),
            (has_zu, has_zu, "slabs", zu), (has_zd, has_zd, "slabs", zd)):
        @pl.when(says)
        def _():
            pl.semaphore_signal(barrier, inc=1, device_id={axis: index}, device_id_type=MESH)
        count = count + hears.astype(jnp.int32)
    ends = jnp.logical_or(row == 0, row == rows - 1)

    @pl.when(ends)
    def _():
        pl.semaphore_signal(barrier, inc=1, device_id={"rows": rows - 1 - row}, device_id_type=MESH)
    pl.semaphore_wait(barrier, count + ends.astype(jnp.int32))

    for load in load_ends:
        load.wait()

    @pl.when(has_up)
    def _():
        each(CHUNKS, lambda k: y_up(0, k).start())

    @pl.when(has_dn)
    def _():
        each(CHUNKS, lambda k: y_dn(0, k).start())

    zeros = jnp.zeros((nz, nl), jnp.float32)

    @pl.when(jnp.logical_not(has_dn))
    def _():
        def clear(x):
            ylo[0, x] = zeros
            ylo[1, x] = zeros
        each(nx, clear)

    @pl.when(jnp.logical_not(has_up))
    def _():
        def clear(x):
            yhi[0, x] = zeros
            yhi[1, x] = zeros
        each(nx, clear)

    for there, ref in ((has_xd, xlo), (has_xu, xhi), (has_zd, zlo), (has_zu, zhi)):
        @pl.when(jnp.logical_not(there))
        def _():
            ref[...] = jnp.zeros_like(ref)

    load_t.wait()

    def stage(x):
        for y in range(ny):
            zsl[0, y, pl.ds(x, 1), :] = out_t[y, x, 0:1, :]
            zsh[0, y, pl.ds(x, 1), :] = out_t[y, x, nz - 1:nz, :]
    each(nx, stage)
    start_sides(0)
    load_c.wait()

    def update(n, x, y, left, right, values, low, high):
        now = n % 2
        v = values[y]
        total = left + right
        lower = jnp.where(first, zlo[now, y, pl.ds(x, 1), :], pltpu.roll(v, 1, 0))
        upper = jnp.where(final, zhi[now, y, pl.ds(x, 1), :], pltpu.roll(v, nz - 1, 0))
        total = total + (lower + upper)
        for other_y in (low, high):
            if other_y is not None:
                total = total + other_y
        return v * (0.6 - 0.2 * (out_c[y, x] * v)) + 0.1 * total

    def over_rows(k, body, n):
        src = fields[n % 2]
        now = n % 2
        low = jnp.maximum(k * width, 1)
        high = jnp.minimum((k + 1) * width, nx - 1)

        @pl.when(k == 0)
        def _():
            body(0, lambda y: xlo[now, y], lambda y: src[y, 1])

        each(high, lambda x: body(x, lambda y: src[y, x - 1], lambda y: src[y, x + 1]), low)

        @pl.when(k == CHUNKS - 1)
        def _():
            body(nx - 1, lambda y: src[y, nx - 2], lambda y: xhi[now, y])

    for n in range(STEPS - 1):
        src, dst = fields[n % 2], fields[(n + 1) % 2]
        now, later = n % 2, (n + 1) % 2
        if n >= 1:
            wait_side_sends(n - 1)
        wait_side_recvs(n)
        if n == 0:
            for late, copy in ((late_xu, x_up), (late_xd, x_dn)):
                @pl.when(late)
                def _():
                    copy(0).start()

        def one_row(x, left, right, n=n, src=src, dst=dst, now=now, later=later):
            values = [src[y, x] for y in range(ny)]
            for y in range(ny):
                below = values[y - 1] if y > 0 else ylo[now, x]
                above = values[y + 1] if y < ny - 1 else yhi[now, x]
                new = update(n, x, y, left(y), right(y), values, below, above)
                dst[y, x] = new
                zsl[later, y, pl.ds(x, 1), :] = new[0:1]
                zsh[later, y, pl.ds(x, 1), :] = new[nz - 1:nz]

        def one_chunk(k, n=n, one_row=one_row):
            wait_y_recvs(n, k)
            if n >= 1:
                wait_y_sends(n - 1, k)
            over_rows(k, one_row, n)
            goes_up = has_up if n + 1 < STEPS - 1 else jnp.logical_and(has_up, k < HELD)

            @pl.when(goes_up)
            def _():
                y_up(n + 1, k).start()

            goes_dn = has_dn if n + 1 < STEPS - 1 else jnp.logical_and(has_dn, k < HELD)

            @pl.when(goes_dn)
            def _():
                y_dn(n + 1, k).start()

        each(CHUNKS, one_chunk)
        start_sides(n + 1)

    n = STEPS - 1
    src, dst = fields[n % 2], fields[(n + 1) % 2]
    wait_side_sends(n - 1)
    wait_side_recvs(n)

    def part_row(x, left, right):
        values = [src[y, x] for y in range(ny)]
        total = 0.1 * values[ny - 1] + inner * values[0]
        for y in range(ny):
            below = values[y - 1] if y > 0 else None
            above = values[y + 1] if y < ny - 1 else None
            new = update(n, x, y, left(y), right(y), values, below, above)
            dst[y, x] = new
            total = total + new
        g[x] = total

    def part_chunk(k):
        wait_y_sends(n - 1, k)
        over_rows(k, part_row, n)
    each(CHUNKS, part_chunk)

    def parts(kind, body):
        each(sets[kind][1], lambda i: body(kind, i))

    def over(kind, i, body):
        start, _, piece, _ = sets[kind]
        each(start + (i + 1) * piece, body, start + i * piece)

    def send(copy):
        return lambda kind, i: copy(kind, i).start()

    def rest_up():
        each(TAILS, lambda j: tail_up(j).start())

    def rest_dn():
        each(TAILS, lambda j: tail_dn(j).start())

    @pl.when(row == 0)
    def _():
        parts(0, send(q_dn))
        parts(2, send(q_up))
        parts(1, send(q_up))
        rest_up()

        def around(kind, i):
            q_dn(kind, i).wait_recv()

            def add(x):
                qd[x] = qd[x] + g[x]
            over(kind, i, add)
            q_dn(kind, i, qd).start()
        parts(1, around)
        parts(2, around)

    @pl.when(row == 1)
    def _():
        parts(1, send(q_dn))
        parts(0, send(q_up))

        def both(kind, i):
            q_up(kind, i).wait_recv()
            q_dn(kind, i).wait_recv()

            def add(x):
                own = g[x]
                qd[x] = qd[x] + own
                g[x] = qu[x] + own
            over(kind, i, add)
            q_up(kind, i).start()
            q_dn(kind, i, qd).start()
        parts(2, both)
        rest_up()
        rest_dn()
        parts(1, lambda kind, i: q_up(kind, i).wait_recv())
        parts(0, lambda kind, i: q_dn(kind, i).wait_recv())

    @pl.when(row == 2)
    def _():
        parts(2, send(q_dn))
        parts(1, send(q_up))

        def both(kind, i):
            q_up(kind, i).wait_recv()

            def add(x):
                g[x] = qu[x] + g[x]
            over(kind, i, add)
            q_up(kind, i).start()
            q_dn(kind, i).wait_recv()
            q_dn(kind, i, qd).start()
        parts(0, both)
        rest_up()
        rest_dn()
        parts(1, lambda kind, i: q_dn(kind, i).wait_recv())
        parts(2, lambda kind, i: q_up(kind, i).wait_recv())

    @pl.when(row == 3)
    def _():
        def forward(kind, i):
            q_dn(kind, i).wait_recv()
            q_dn(kind, i, qd).start()
        parts(0, forward)
        parts(1, forward)
        rest_dn()
        parts(0, lambda kind, i: q_up(kind, i).wait_recv())
        parts(1, lambda kind, i: q_up(kind, i).wait_recv())
        parts(2, lambda kind, i: q_dn(kind, i).wait_recv())

    scale = 1.0 / (ny * rows)

    def end_row(x):
        low = ylo[n % 2, x]
        kind = (x >= sets[1][0]).astype(jnp.int32) + (x >= sets[2][0]).astype(jnp.int32)
        use_u = jnp.logical_and(has_dn, kind != row - 1)
        use_d = jnp.logical_and(has_dn, kind <= row - 1)
        sums = lax.select(use_u, qu[x], zeros) + lax.select(use_d, qd[x], zeros)
        sums = sums + inner * (src[0, x] - low)
        for y in range(ny):
            value = dst[y, x]
            if y == 0:
                value = value + 0.1 * low
            if y == ny - 1:
                value = value + 0.1 * yhi[n % 2, x]
            if y in (0, ny - 1):
                dst[y, x] = value
            sums = sums + value
            out_c[y, x] = sums * scale

    def end_chunk(k):
        wait_y_recvs(n, k)
        each((k + 1) * width, end_row, k * width)
    each(HELD, end_chunk)

    def end_tail(j):
        @pl.when(has_dn)
        def _():
            tail_up(j).wait_recv()

        @pl.when(has_up)
        def _():
            tail_dn(j).wait_recv()
        size = (nx - HELD * width) // TAILS
        each(HELD * width + (j + 1) * size, end_row, HELD * width + j * size)
    each(TAILS, end_tail)

    each(HELD, lambda k: wait_y_sends(n, k))

    @pl.when(has_up)
    def _():
        each(TAILS, lambda j: tail_up(j).wait_send())

    @pl.when(has_dn)
    def _():
        each(TAILS, lambda j: tail_dn(j).wait_send())
    wait_side_sends(n)

    for r in range(rows):
        @pl.when(row == r)
        def _():
            for kind in range(3):
                if r < rows - 1 and kind != r:
                    parts(kind, lambda kind, i: q_up(kind, i).wait_send())
                if kind not in {0: (), 1: (0,), 2: (1,), 3: (2,)}[r]:
                    parts(kind, lambda kind, i: q_dn(kind, i).wait_send())


def write(c_ref, t_ref, out_c, out_t, sem):
    copies = []
    for i, (src, dst) in enumerate(((c_ref, out_c), (t_ref, out_t))):
        for j in range(WRITES):
            width = src.shape[1] // WRITES
            at = (slice(None), pl.ds(j * width, width)) if WRITES > src.shape[0] else (pl.ds(j * (src.shape[0] // WRITES), src.shape[0] // WRITES),)
            copies.append(pltpu.make_async_copy(src.at[at], dst.at[at], sem.at[i, j]))
    for copy in copies:
        copy.start()
    for copy in copies:
        copy.wait()


def body(tracer, crowding):
    ny, nx, nz, nl = tracer.shape
    sizes = tuple(lax.axis_size(a) for a in ("rows", "cols", "slabs"))
    shape = jax.ShapeDtypeStruct(tracer.shape, jnp.float32)
    vmem = lambda *s: pltpu.VMEM(s, jnp.float32)
    dma = pltpu.SemaphoreType.DMA
    parts = sum(count for _, count, _, _ in column_sets(nx))
    sums, field = pl.pallas_call(
        functools.partial(kernel, sizes),
        out_shape=(shape, shape),
        in_specs=[pl.BlockSpec(memory_space=pltpu.HBM)] * 2,
        out_specs=[pl.BlockSpec(memory_space=pltpu.VMEM)] * 2,
        scratch_shapes=[
            vmem(ny, nx, nz, nl),
            vmem(2, nx, nz, nl), vmem(2, nx, nz, nl),
            vmem(2, ny, nz, nl), vmem(2, ny, nz, nl),
            vmem(2, ny, nx, nl), vmem(2, ny, nx, nl),
            vmem(2, ny, nx, nl), vmem(2, ny, nx, nl),
            vmem(nx, nz, nl), vmem(nx, nz, nl), vmem(nx, nz, nl),
            dma((4,)),
            dma((STEPS, CHUNKS)), dma((STEPS, CHUNKS)), dma((STEPS, CHUNKS)), dma((STEPS, CHUNKS)),
            dma((STEPS, 2)), dma((STEPS, 2)), dma((STEPS, 2)), dma((STEPS, 2)),
            dma((parts,)), dma((parts,)), dma((parts,)), dma((parts,)),
            dma((2, TAILS)), dma((2, TAILS)),
        ],
        compiler_params=pltpu.CompilerParams(
            collective_id=0, has_side_effects=True, vmem_limit_bytes=30 * 1024 * 1024),
        name="grid_steps",
    )(tracer, crowding)
    return pl.pallas_call(
        write,
        out_shape=(shape, shape),
        in_specs=[pl.BlockSpec(memory_space=pltpu.VMEM)] * 2,
        out_specs=[pl.BlockSpec(memory_space=pltpu.HBM)] * 2,
        scratch_shapes=[dma((2, WRITES))],
        compiler_params=pltpu.CompilerParams(vmem_limit_bytes=1024 * 1024),
        name="write_out",
    )(sums, field)


def solution(mesh):
    placed = P("rows", "cols", "slabs", None)
    return jax.shard_map(body, mesh=mesh, in_specs=(placed, placed), out_specs=(placed, placed), check_vma=False)
```

```python
import functools

import jax
import jax.numpy as jnp
from jax import lax
from jax.experimental import pallas as pl
from jax.experimental.pallas import tpu as pltpu
from jax.sharding import PartitionSpec as P

STEPS = 4
CHUNKS = 2
HELD = 1
TAILS = 4
WRITES = 4
SHARES = ((21, 22, 21), (22, 21, 21))
MESH = pl.DeviceIdType.MESH


def column_sets(nx, shares):
    counts = [share * nx // sum(shares) for share in shares]
    counts[2] = nx - counts[0] - counts[1]
    sets, start, base = [], 0, 0
    for count in counts:
        piece = next(p for p in (11, 7, 6, 5, 4, 3, 2, 1) if count % p == 0)
        sets.append((start, count // piece, piece, base))
        start, base = start + count, base + count // piece
    return sets


def kernel(sizes, tr, cr, out_c, out_t, other, ylo, yhi, xlo, xhi, zlo, zhi, zsl, zsh, qu, qd, g,
           load_sem, yu_s, yu_r, yd_s, yd_r, xs, xr, zs, zr, qu_s, qu_r, qd_s, qd_r, tail_s, tail_r):
    rows, cols, slabs = sizes
    ny, nx, nz, nl = tr.shape
    width = nx // CHUNKS
    row, col, slab = (lax.axis_index(a) for a in ("rows", "cols", "slabs"))
    has_up, has_dn = row < rows - 1, row > 0
    has_xu, has_xd = col < cols - 1, col > 0
    has_zu, has_zd = slab < slabs - 1, slab > 0
    fields = (out_t, other)
    first = lax.broadcasted_iota(jnp.int32, (nz, nl), 0) == 0
    final = lax.broadcasted_iota(jnp.int32, (nz, nl), 0) == nz - 1
    inner = jnp.where(has_dn, jnp.float32(0.1), jnp.float32(0.0))

    early = slab < slabs // 2
    below_middle, above_middle = col == cols // 2 - 1, col == cols // 2
    late_xu = jnp.logical_and(below_middle, early)
    late_xd = jnp.logical_and(above_middle, jnp.logical_not(early))
    quiet_xu = jnp.logical_and(below_middle, jnp.logical_not(early))
    quiet_xd = jnp.logical_and(above_middle, early)

    def both_but(a, b):
        return jnp.logical_and(a, jnp.logical_not(b))

    def chunk(k):
        return pl.ds(pl.multiple_of(k * width, width), width)

    def remote(src, dst, send, recv, axis, index):
        return pltpu.make_async_remote_copy(
            src_ref=src, dst_ref=dst, send_sem=send, recv_sem=recv,
            device_id={axis: index}, device_id_type=MESH)

    up, dn, back = jnp.minimum(row + 1, rows - 1), jnp.maximum(row - 1, 0), lax.rem(row + rows - 1, rows)
    choices = [column_sets(nx, shares) for shares in SHARES]
    sets = list(choices[0])
    core = lax.rem(slab, len(choices))
    xu, xd = jnp.minimum(col + 1, cols - 1), jnp.maximum(col - 1, 0)
    zu, zd = jnp.minimum(slab + 1, slabs - 1), jnp.maximum(slab - 1, 0)

    def y_up(n, k):
        return remote(fields[n % 2].at[ny - 1, chunk(k)], ylo.at[n % 2, chunk(k)], yu_s.at[n, k], yu_r.at[n, k], "rows", up)

    def y_dn(n, k):
        return remote(fields[n % 2].at[0, chunk(k)], yhi.at[n % 2, chunk(k)], yd_s.at[n, k], yd_r.at[n, k], "rows", dn)

    def tail(j):
        start = HELD * width
        size = (nx - start) // TAILS
        return pl.ds(start + j * size, size)

    def tail_up(j):
        here = fields[(STEPS - 1) % 2].at[ny - 1, tail(j)]
        return remote(here, ylo.at[(STEPS - 1) % 2, tail(j)], tail_s.at[0, j], tail_r.at[0, j], "rows", up)

    def tail_dn(j):
        here = fields[(STEPS - 1) % 2].at[0, tail(j)]
        return remote(here, yhi.at[(STEPS - 1) % 2, tail(j)], tail_s.at[1, j], tail_r.at[1, j], "rows", dn)

    def x_up(n):
        return remote(fields[n % 2].at[:, nx - 1], xlo.at[n % 2], xs.at[n, 0], xr.at[n, 0], "cols", xu)

    def x_dn(n):
        return remote(fields[n % 2].at[:, 0], xhi.at[n % 2], xs.at[n, 1], xr.at[n, 1], "cols", xd)

    def z_up(n):
        return remote(zsh.at[n % 2], zlo.at[n % 2], zs.at[n, 0], zr.at[n, 0], "slabs", zu)

    def z_dn(n):
        return remote(zsl.at[n % 2], zhi.at[n % 2], zs.at[n, 1], zr.at[n, 1], "slabs", zd)

    def part(kind, i):
        start, _, piece, _ = sets[kind]
        return pl.ds(start + i * piece, piece)

    def q_up(kind, i):
        j = sets[kind][3] + i
        return remote(g.at[part(kind, i)], qu.at[part(kind, i)], qu_s.at[j], qu_r.at[j], "rows", up)

    def q_dn(kind, i, src=g):
        j = sets[kind][3] + i
        return remote(src.at[part(kind, i)], qd.at[part(kind, i)], qd_s.at[j], qd_r.at[j], "rows", back)

    sides = ((has_xu, has_xd, x_up), (has_xd, has_xu, x_dn), (has_zu, has_zd, z_up), (has_zd, has_zu, z_dn))

    def start_sides(n):
        for sends, _, copy in sides:
            if n == 0 and copy is x_up:
                sends = both_but(sends, late_xu)
            if n == 0 and copy is x_dn:
                sends = both_but(sends, late_xd)

            @pl.when(sends)
            def _():
                copy(n).start()

    def wait_side_sends(n):
        for sends, _, copy in sides:
            @pl.when(sends)
            def _():
                copy(n).wait_send()

    def wait_side_recvs(n):
        for _, gets, copy in sides:
            @pl.when(gets)
            def _():
                copy(n).wait_recv()

    def wait_y_sends(n, k):
        @pl.when(has_up)
        def _():
            y_up(n, k).wait_send()

        @pl.when(has_dn)
        def _():
            y_dn(n, k).wait_send()

    def wait_y_recvs(n, k):
        @pl.when(has_dn)
        def _():
            y_up(n, k).wait_recv()

        @pl.when(has_up)
        def _():
            y_dn(n, k).wait_recv()

    def each(count, body, start=0):
        def turn(i, carry):
            body(i)
            return carry
        lax.fori_loop(start, count, turn, 0)

    inside = pl.ds(1, ny - 2)
    load_ends = [pltpu.make_async_copy(tr.at[y], out_t.at[y], load_sem.at[i]) for i, y in enumerate((0, ny - 1))]
    load_t = pltpu.make_async_copy(tr.at[inside], out_t.at[inside], load_sem.at[2])
    load_c = pltpu.make_async_copy(cr, out_c, load_sem.at[3])
    for load in load_ends:
        load.start()
    load_t.start()
    load_c.start()

    barrier = pltpu.get_barrier_semaphore()
    count = jnp.int32(0)
    for says, hears, axis, index in (
            (has_up, has_up, "rows", up), (has_dn, has_dn, "rows", dn),
            (both_but(has_xu, quiet_xu), both_but(has_xu, late_xu), "cols", xu),
            (both_but(has_xd, quiet_xd), both_but(has_xd, late_xd), "cols", xd),
            (has_zu, has_zu, "slabs", zu), (has_zd, has_zd, "slabs", zd)):
        @pl.when(says)
        def _():
            pl.semaphore_signal(barrier, inc=1, device_id={axis: index}, device_id_type=MESH)
        count = count + hears.astype(jnp.int32)
    ends = jnp.logical_or(row == 0, row == rows - 1)

    @pl.when(ends)
    def _():
        pl.semaphore_signal(barrier, inc=1, device_id={"rows": rows - 1 - row}, device_id_type=MESH)
    pl.semaphore_wait(barrier, count + ends.astype(jnp.int32))

    for load in load_ends:
        load.wait()

    @pl.when(has_up)
    def _():
        each(CHUNKS, lambda k: y_up(0, k).start())

    @pl.when(has_dn)
    def _():
        each(CHUNKS, lambda k: y_dn(0, k).start())

    zeros = jnp.zeros((nz, nl), jnp.float32)

    @pl.when(jnp.logical_not(has_dn))
    def _():
        def clear(x):
            ylo[0, x] = zeros
            ylo[1, x] = zeros
        each(nx, clear)

    @pl.when(jnp.logical_not(has_up))
    def _():
        def clear(x):
            yhi[0, x] = zeros
            yhi[1, x] = zeros
        each(nx, clear)

    for there, ref in ((has_xd, xlo), (has_xu, xhi), (has_zd, zlo), (has_zu, zhi)):
        @pl.when(jnp.logical_not(there))
        def _():
            ref[...] = jnp.zeros_like(ref)

    load_t.wait()

    def stage(x):
        for y in range(ny):
            zsl[0, y, pl.ds(x, 1), :] = out_t[y, x, 0:1, :]
            zsh[0, y, pl.ds(x, 1), :] = out_t[y, x, nz - 1:nz, :]
    each(nx, stage)
    start_sides(0)
    load_c.wait()

    def update(n, x, y, left, right, values, low, high):
        now = n % 2
        v = values[y]
        total = left + right
        lower = jnp.where(first, zlo[now, y, pl.ds(x, 1), :], pltpu.roll(v, 1, 0))
        upper = jnp.where(final, zhi[now, y, pl.ds(x, 1), :], pltpu.roll(v, nz - 1, 0))
        total = total + (lower + upper)
        for other_y in (low, high):
            if other_y is not None:
                total = total + other_y
        return v * (0.6 - 0.2 * (out_c[y, x] * v)) + 0.1 * total

    def over_rows(k, body, n):
        src = fields[n % 2]
        now = n % 2
        low = jnp.maximum(k * width, 1)
        high = jnp.minimum((k + 1) * width, nx - 1)

        @pl.when(k == 0)
        def _():
            body(0, lambda y: xlo[now, y], lambda y: src[y, 1])

        each(high, lambda x: body(x, lambda y: src[y, x - 1], lambda y: src[y, x + 1]), low)

        @pl.when(k == CHUNKS - 1)
        def _():
            body(nx - 1, lambda y: src[y, nx - 2], lambda y: xhi[now, y])

    for n in range(STEPS - 1):
        src, dst = fields[n % 2], fields[(n + 1) % 2]
        now, later = n % 2, (n + 1) % 2
        if n >= 1:
            wait_side_sends(n - 1)
        wait_side_recvs(n)
        if n == 0:
            for late, copy in ((late_xu, x_up), (late_xd, x_dn)):
                @pl.when(late)
                def _():
                    copy(0).start()

        def one_row(x, left, right, n=n, src=src, dst=dst, now=now, later=later):
            values = [src[y, x] for y in range(ny)]
            for y in range(ny):
                below = values[y - 1] if y > 0 else ylo[now, x]
                above = values[y + 1] if y < ny - 1 else yhi[now, x]
                new = update(n, x, y, left(y), right(y), values, below, above)
                dst[y, x] = new
                zsl[later, y, pl.ds(x, 1), :] = new[0:1]
                zsh[later, y, pl.ds(x, 1), :] = new[nz - 1:nz]

        def one_chunk(k, n=n, one_row=one_row):
            wait_y_recvs(n, k)
            if n >= 1:
                wait_y_sends(n - 1, k)
            over_rows(k, one_row, n)
            goes_up = has_up if n + 1 < STEPS - 1 else jnp.logical_and(has_up, k < HELD)

            @pl.when(goes_up)
            def _():
                y_up(n + 1, k).start()

            goes_dn = has_dn if n + 1 < STEPS - 1 else jnp.logical_and(has_dn, k < HELD)

            @pl.when(goes_dn)
            def _():
                y_dn(n + 1, k).start()

        each(CHUNKS, one_chunk)
        start_sides(n + 1)

    n = STEPS - 1
    src, dst = fields[n % 2], fields[(n + 1) % 2]
    wait_side_sends(n - 1)
    wait_side_recvs(n)

    def part_row(x, left, right):
        values = [src[y, x] for y in range(ny)]
        total = 0.1 * values[ny - 1] + inner * values[0]
        for y in range(ny):
            below = values[y - 1] if y > 0 else None
            above = values[y + 1] if y < ny - 1 else None
            new = update(n, x, y, left(y), right(y), values, below, above)
            dst[y, x] = new
            total = total + new
        g[x] = total

    def part_chunk(k):
        wait_y_sends(n - 1, k)
        over_rows(k, part_row, n)
    each(CHUNKS, part_chunk)

    def parts(kind, body):
        each(sets[kind][1], lambda i: body(kind, i))

    def over(kind, i, body):
        start, _, piece, _ = sets[kind]
        each(start + (i + 1) * piece, body, start + i * piece)

    def send(copy):
        return lambda kind, i: copy(kind, i).start()

    def rest_up():
        each(TAILS, lambda j: tail_up(j).start())

    def rest_dn():
        each(TAILS, lambda j: tail_dn(j).start())

    for which, choice in enumerate(choices):
        sets[:] = choice

        @pl.when(jnp.logical_and(core == which, row == 0))
        def _():
            parts(0, send(q_dn))
            parts(2, send(q_up))
            parts(1, send(q_up))
            rest_up()

            def around(kind, i):
                q_dn(kind, i).wait_recv()

                def add(x):
                    qd[x] = qd[x] + g[x]
                over(kind, i, add)
                q_dn(kind, i, qd).start()
            parts(1, around)
            parts(2, around)

        @pl.when(jnp.logical_and(core == which, row == 1))
        def _():
            parts(1, send(q_dn))
            parts(0, send(q_up))

            def both(kind, i):
                q_up(kind, i).wait_recv()
                q_dn(kind, i).wait_recv()

                def add(x):
                    own = g[x]
                    qd[x] = qd[x] + own
                    g[x] = qu[x] + own
                over(kind, i, add)
                q_up(kind, i).start()
                q_dn(kind, i, qd).start()
            parts(2, both)
            rest_up()
            rest_dn()
            parts(1, lambda kind, i: q_up(kind, i).wait_recv())
            parts(0, lambda kind, i: q_dn(kind, i).wait_recv())

        @pl.when(jnp.logical_and(core == which, row == 2))
        def _():
            parts(2, send(q_dn))
            parts(1, send(q_up))

            def both(kind, i):
                q_up(kind, i).wait_recv()

                def add(x):
                    g[x] = qu[x] + g[x]
                over(kind, i, add)
                q_up(kind, i).start()
                q_dn(kind, i).wait_recv()
                q_dn(kind, i, qd).start()
            parts(0, both)
            rest_up()
            rest_dn()
            parts(1, lambda kind, i: q_dn(kind, i).wait_recv())
            parts(2, lambda kind, i: q_up(kind, i).wait_recv())

        @pl.when(jnp.logical_and(core == which, row == 3))
        def _():
            def forward(kind, i):
                q_dn(kind, i).wait_recv()
                q_dn(kind, i, qd).start()
            parts(0, forward)
            parts(1, forward)
            rest_dn()
            parts(0, lambda kind, i: q_up(kind, i).wait_recv())
            parts(1, lambda kind, i: q_up(kind, i).wait_recv())
            parts(2, lambda kind, i: q_dn(kind, i).wait_recv())

    scale = 1.0 / (ny * rows)

    cuts = [jnp.where(core == 0, choices[0][kind][0], choices[1][kind][0]) for kind in (1, 2)]

    def end_row(x):
        low = ylo[n % 2, x]
        kind = (x >= cuts[0]).astype(jnp.int32) + (x >= cuts[1]).astype(jnp.int32)
        use_u = jnp.logical_and(has_dn, kind != row - 1)
        use_d = jnp.logical_and(has_dn, kind <= row - 1)
        sums = lax.select(use_u, qu[x], zeros) + lax.select(use_d, qd[x], zeros)
        sums = sums + inner * (src[0, x] - low)
        for y in range(ny):
            value = dst[y, x]
            if y == 0:
                value = value + 0.1 * low
            if y == ny - 1:
                value = value + 0.1 * yhi[n % 2, x]
            if y in (0, ny - 1):
                dst[y, x] = value
            sums = sums + value
            out_c[y, x] = sums * scale

    def end_chunk(k):
        wait_y_recvs(n, k)
        each((k + 1) * width, end_row, k * width)
    each(HELD, end_chunk)

    def end_tail(j):
        @pl.when(has_dn)
        def _():
            tail_up(j).wait_recv()

        @pl.when(has_up)
        def _():
            tail_dn(j).wait_recv()
        size = (nx - HELD * width) // TAILS
        each(HELD * width + (j + 1) * size, end_row, HELD * width + j * size)
    each(TAILS, end_tail)

    each(HELD, lambda k: wait_y_sends(n, k))

    @pl.when(has_up)
    def _():
        each(TAILS, lambda j: tail_up(j).wait_send())

    @pl.when(has_dn)
    def _():
        each(TAILS, lambda j: tail_dn(j).wait_send())
    wait_side_sends(n)

    for which, choice in enumerate(choices):
        sets[:] = choice
        for r in range(rows):
            @pl.when(jnp.logical_and(core == which, row == r))
            def _():
                for kind in range(3):
                    if r < rows - 1 and kind != r:
                        parts(kind, lambda kind, i: q_up(kind, i).wait_send())
                    if kind not in {0: (), 1: (0,), 2: (1,), 3: (2,)}[r]:
                        parts(kind, lambda kind, i: q_dn(kind, i).wait_send())


def write(c_ref, t_ref, out_c, out_t, sem):
    copies = []
    for i, (src, dst) in enumerate(((c_ref, out_c), (t_ref, out_t))):
        for j in range(WRITES):
            width = src.shape[1] // WRITES
            at = (slice(None), pl.ds(j * width, width)) if WRITES > src.shape[0] else (pl.ds(j * (src.shape[0] // WRITES), src.shape[0] // WRITES),)
            copies.append(pltpu.make_async_copy(src.at[at], dst.at[at], sem.at[i, j]))
    for copy in copies:
        copy.start()
    for copy in copies:
        copy.wait()


def body(tracer, crowding):
    ny, nx, nz, nl = tracer.shape
    sizes = tuple(lax.axis_size(a) for a in ("rows", "cols", "slabs"))
    shape = jax.ShapeDtypeStruct(tracer.shape, jnp.float32)
    vmem = lambda *s: pltpu.VMEM(s, jnp.float32)
    dma = pltpu.SemaphoreType.DMA
    parts = max(sum(count for _, count, _, _ in column_sets(nx, shares)) for shares in SHARES)
    sums, field = pl.pallas_call(
        functools.partial(kernel, sizes),
        out_shape=(shape, shape),
        in_specs=[pl.BlockSpec(memory_space=pltpu.HBM)] * 2,
        out_specs=[pl.BlockSpec(memory_space=pltpu.VMEM)] * 2,
        scratch_shapes=[
            vmem(ny, nx, nz, nl),
            vmem(2, nx, nz, nl), vmem(2, nx, nz, nl),
            vmem(2, ny, nz, nl), vmem(2, ny, nz, nl),
            vmem(2, ny, nx, nl), vmem(2, ny, nx, nl),
            vmem(2, ny, nx, nl), vmem(2, ny, nx, nl),
            vmem(nx, nz, nl), vmem(nx, nz, nl), vmem(nx, nz, nl),
            dma((4,)),
            dma((STEPS, CHUNKS)), dma((STEPS, CHUNKS)), dma((STEPS, CHUNKS)), dma((STEPS, CHUNKS)),
            dma((STEPS, 2)), dma((STEPS, 2)), dma((STEPS, 2)), dma((STEPS, 2)),
            dma((parts,)), dma((parts,)), dma((parts,)), dma((parts,)),
            dma((2, TAILS)), dma((2, TAILS)),
        ],
        compiler_params=pltpu.CompilerParams(
            collective_id=0, has_side_effects=True, vmem_limit_bytes=30 * 1024 * 1024),
        name="grid_steps",
    )(tracer, crowding)
    return pl.pallas_call(
        write,
        out_shape=(shape, shape),
        in_specs=[pl.BlockSpec(memory_space=pltpu.VMEM)] * 2,
        out_specs=[pl.BlockSpec(memory_space=pltpu.HBM)] * 2,
        scratch_shapes=[dma((2, WRITES))],
        compiler_params=pltpu.CompilerParams(vmem_limit_bytes=1024 * 1024),
        name="write_out",
    )(sums, field)


def solution(mesh):
    placed = P("rows", "cols", "slabs", None)
    return jax.shard_map(body, mesh=mesh, in_specs=(placed, placed), out_specs=(placed, placed), check_vma=False)
```

```python
import functools

import jax
import jax.numpy as jnp
from jax import lax
from jax.experimental import pallas as pl
from jax.experimental.pallas import tpu as pltpu
from jax.sharding import PartitionSpec as P

STEPS = 4
CHUNKS = 2
HELD = 1
TAILS = 2
WRITES = 4
SHARES = ((21, 22, 21), (22, 21, 21))
MESH = pl.DeviceIdType.MESH


def column_sets(nx, shares):
    counts = [share * nx // sum(shares) for share in shares]
    counts[2] = nx - counts[0] - counts[1]
    sets, start, base = [], 0, 0
    for count in counts:
        piece = next(p for p in (11, 7, 6, 5, 4, 3, 2, 1) if count % p == 0)
        sets.append((start, count // piece, piece, base))
        start, base = start + count, base + count // piece
    return sets


def kernel(sizes, tr, cr, out_c, out_t, other, ylo, yhi, xlo, xhi, zlo, zhi, zsl, zsh, qu, qd, g,
           load_sem, yu_s, yu_r, yd_s, yd_r, xs, xr, zs, zr, qu_s, qu_r, qd_s, qd_r, tail_s, tail_r):
    rows, cols, slabs = sizes
    ny, nx, nz, nl = tr.shape
    width = nx // CHUNKS
    row, col, slab = (lax.axis_index(a) for a in ("rows", "cols", "slabs"))
    has_up, has_dn = row < rows - 1, row > 0
    has_xu, has_xd = col < cols - 1, col > 0
    has_zu, has_zd = slab < slabs - 1, slab > 0
    fields = (out_t, other)
    first = lax.broadcasted_iota(jnp.int32, (nz, nl), 0) == 0
    final = lax.broadcasted_iota(jnp.int32, (nz, nl), 0) == nz - 1
    inner = jnp.where(has_dn, jnp.float32(0.1), jnp.float32(0.0))

    early = slab < slabs // 2
    below_middle, above_middle = col == cols // 2 - 1, col == cols // 2
    late_xu = jnp.logical_and(below_middle, early)
    late_xd = jnp.logical_and(above_middle, jnp.logical_not(early))
    quiet_xu = jnp.logical_and(below_middle, jnp.logical_not(early))
    quiet_xd = jnp.logical_and(above_middle, early)

    def both_but(a, b):
        return jnp.logical_and(a, jnp.logical_not(b))

    def chunk(k):
        return pl.ds(pl.multiple_of(k * width, width), width)

    def remote(src, dst, send, recv, axis, index):
        return pltpu.make_async_remote_copy(
            src_ref=src, dst_ref=dst, send_sem=send, recv_sem=recv,
            device_id={axis: index}, device_id_type=MESH)

    up, dn, back = jnp.minimum(row + 1, rows - 1), jnp.maximum(row - 1, 0), lax.rem(row + rows - 1, rows)
    choices = [column_sets(nx, shares) for shares in SHARES]
    sets = list(choices[0])
    core = lax.rem(slab, len(choices))
    xu, xd = jnp.minimum(col + 1, cols - 1), jnp.maximum(col - 1, 0)
    zu, zd = jnp.minimum(slab + 1, slabs - 1), jnp.maximum(slab - 1, 0)

    def y_up(n, k):
        return remote(fields[n % 2].at[ny - 1, chunk(k)], ylo.at[n % 2, chunk(k)], yu_s.at[n, k], yu_r.at[n, k], "rows", up)

    def y_dn(n, k):
        return remote(fields[n % 2].at[0, chunk(k)], yhi.at[n % 2, chunk(k)], yd_s.at[n, k], yd_r.at[n, k], "rows", dn)

    def tail(j):
        start = HELD * width
        size = (nx - start) // TAILS
        return pl.ds(start + j * size, size)

    def tail_up(j):
        here = fields[(STEPS - 1) % 2].at[ny - 1, tail(j)]
        return remote(here, ylo.at[(STEPS - 1) % 2, tail(j)], tail_s.at[0, j], tail_r.at[0, j], "rows", up)

    def tail_dn(j):
        here = fields[(STEPS - 1) % 2].at[0, tail(j)]
        return remote(here, yhi.at[(STEPS - 1) % 2, tail(j)], tail_s.at[1, j], tail_r.at[1, j], "rows", dn)

    def x_up(n):
        return remote(fields[n % 2].at[:, nx - 1], xlo.at[n % 2], xs.at[n, 0], xr.at[n, 0], "cols", xu)

    def x_dn(n):
        return remote(fields[n % 2].at[:, 0], xhi.at[n % 2], xs.at[n, 1], xr.at[n, 1], "cols", xd)

    def z_up(n):
        return remote(zsh.at[n % 2], zlo.at[n % 2], zs.at[n, 0], zr.at[n, 0], "slabs", zu)

    def z_dn(n):
        return remote(zsl.at[n % 2], zhi.at[n % 2], zs.at[n, 1], zr.at[n, 1], "slabs", zd)

    def part(kind, i):
        start, _, piece, _ = sets[kind]
        return pl.ds(start + i * piece, piece)

    def q_up(kind, i):
        j = sets[kind][3] + i
        return remote(g.at[part(kind, i)], qu.at[part(kind, i)], qu_s.at[j], qu_r.at[j], "rows", up)

    def q_dn(kind, i, src=g):
        j = sets[kind][3] + i
        return remote(src.at[part(kind, i)], qd.at[part(kind, i)], qd_s.at[j], qd_r.at[j], "rows", back)

    sides = ((has_xu, has_xd, x_up), (has_xd, has_xu, x_dn), (has_zu, has_zd, z_up), (has_zd, has_zu, z_dn))

    def start_sides(n):
        for sends, _, copy in sides:
            if n == 0 and copy is x_up:
                sends = both_but(sends, late_xu)
            if n == 0 and copy is x_dn:
                sends = both_but(sends, late_xd)

            @pl.when(sends)
            def _():
                copy(n).start()

    def wait_side_sends(n):
        for sends, _, copy in sides:
            @pl.when(sends)
            def _():
                copy(n).wait_send()

    def wait_side_recvs(n):
        for _, gets, copy in sides:
            @pl.when(gets)
            def _():
                copy(n).wait_recv()

    def wait_y_sends(n, k):
        @pl.when(has_up)
        def _():
            y_up(n, k).wait_send()

        @pl.when(has_dn)
        def _():
            y_dn(n, k).wait_send()

    def wait_y_recvs(n, k):
        @pl.when(has_dn)
        def _():
            y_up(n, k).wait_recv()

        @pl.when(has_up)
        def _():
            y_dn(n, k).wait_recv()

    def each(count, body, start=0):
        def turn(i, carry):
            body(i)
            return carry
        lax.fori_loop(start, count, turn, 0)

    inside = pl.ds(1, ny - 2)
    load_ends = [pltpu.make_async_copy(tr.at[y], out_t.at[y], load_sem.at[i]) for i, y in enumerate((0, ny - 1))]
    load_t = pltpu.make_async_copy(tr.at[inside], out_t.at[inside], load_sem.at[2])
    load_c = pltpu.make_async_copy(cr, out_c, load_sem.at[3])
    for load in load_ends:
        load.start()
    load_t.start()
    load_c.start()

    barrier = pltpu.get_barrier_semaphore()
    count = jnp.int32(0)
    for says, hears, axis, index in (
            (has_up, has_up, "rows", up), (has_dn, has_dn, "rows", dn),
            (both_but(has_xu, quiet_xu), both_but(has_xu, late_xu), "cols", xu),
            (both_but(has_xd, quiet_xd), both_but(has_xd, late_xd), "cols", xd),
            (has_zu, has_zu, "slabs", zu), (has_zd, has_zd, "slabs", zd)):
        @pl.when(says)
        def _():
            pl.semaphore_signal(barrier, inc=1, device_id={axis: index}, device_id_type=MESH)
        count = count + hears.astype(jnp.int32)
    ends = jnp.logical_or(row == 0, row == rows - 1)

    @pl.when(ends)
    def _():
        pl.semaphore_signal(barrier, inc=1, device_id={"rows": rows - 1 - row}, device_id_type=MESH)
    pl.semaphore_wait(barrier, count + ends.astype(jnp.int32))

    for load in load_ends:
        load.wait()

    @pl.when(has_up)
    def _():
        each(CHUNKS, lambda k: y_up(0, k).start())

    @pl.when(has_dn)
    def _():
        each(CHUNKS, lambda k: y_dn(0, k).start())

    zeros = jnp.zeros((nz, nl), jnp.float32)

    @pl.when(jnp.logical_not(has_dn))
    def _():
        def clear(x):
            ylo[0, x] = zeros
            ylo[1, x] = zeros
        each(nx, clear)

    @pl.when(jnp.logical_not(has_up))
    def _():
        def clear(x):
            yhi[0, x] = zeros
            yhi[1, x] = zeros
        each(nx, clear)

    for there, ref in ((has_xd, xlo), (has_xu, xhi), (has_zd, zlo), (has_zu, zhi)):
        @pl.when(jnp.logical_not(there))
        def _():
            ref[...] = jnp.zeros_like(ref)

    load_t.wait()

    def stage(x):
        for y in range(ny):
            zsl[0, y, pl.ds(x, 1), :] = out_t[y, x, 0:1, :]
            zsh[0, y, pl.ds(x, 1), :] = out_t[y, x, nz - 1:nz, :]
    each(nx, stage)
    start_sides(0)
    load_c.wait()

    def update(n, x, y, left, right, values, low, high):
        now = n % 2
        v = values[y]
        total = left + right
        lower = jnp.where(first, zlo[now, y, pl.ds(x, 1), :], pltpu.roll(v, 1, 0))
        upper = jnp.where(final, zhi[now, y, pl.ds(x, 1), :], pltpu.roll(v, nz - 1, 0))
        total = total + (lower + upper)
        for other_y in (low, high):
            if other_y is not None:
                total = total + other_y
        return v * (0.6 - 0.2 * (out_c[y, x] * v)) + 0.1 * total

    def over_rows(k, body, n):
        src = fields[n % 2]
        now = n % 2
        low = jnp.maximum(k * width, 1)
        high = jnp.minimum((k + 1) * width, nx - 1)

        @pl.when(k == 0)
        def _():
            body(0, lambda y: xlo[now, y], lambda y: src[y, 1])

        each(high, lambda x: body(x, lambda y: src[y, x - 1], lambda y: src[y, x + 1]), low)

        @pl.when(k == CHUNKS - 1)
        def _():
            body(nx - 1, lambda y: src[y, nx - 2], lambda y: xhi[now, y])

    for n in range(STEPS - 1):
        src, dst = fields[n % 2], fields[(n + 1) % 2]
        now, later = n % 2, (n + 1) % 2
        if n >= 1:
            wait_side_sends(n - 1)
        wait_side_recvs(n)
        if n == 0:
            for late, copy in ((late_xu, x_up), (late_xd, x_dn)):
                @pl.when(late)
                def _():
                    copy(0).start()

        def one_row(x, left, right, n=n, src=src, dst=dst, now=now, later=later):
            values = [src[y, x] for y in range(ny)]
            for y in range(ny):
                below = values[y - 1] if y > 0 else ylo[now, x]
                above = values[y + 1] if y < ny - 1 else yhi[now, x]
                new = update(n, x, y, left(y), right(y), values, below, above)
                dst[y, x] = new
                zsl[later, y, pl.ds(x, 1), :] = new[0:1]
                zsh[later, y, pl.ds(x, 1), :] = new[nz - 1:nz]

        def one_chunk(k, n=n, one_row=one_row):
            wait_y_recvs(n, k)
            if n >= 1:
                wait_y_sends(n - 1, k)
            over_rows(k, one_row, n)
            goes_up = has_up if n + 1 < STEPS - 1 else jnp.logical_and(has_up, k < HELD)

            @pl.when(goes_up)
            def _():
                y_up(n + 1, k).start()

            goes_dn = has_dn if n + 1 < STEPS - 1 else jnp.logical_and(has_dn, k < HELD)

            @pl.when(goes_dn)
            def _():
                y_dn(n + 1, k).start()

        each(CHUNKS, one_chunk)
        start_sides(n + 1)

    n = STEPS - 1
    src, dst = fields[n % 2], fields[(n + 1) % 2]
    wait_side_sends(n - 1)
    wait_side_recvs(n)

    def part_row(x, left, right):
        values = [src[y, x] for y in range(ny)]
        total = 0.1 * values[ny - 1] + inner * values[0]
        for y in range(ny):
            below = values[y - 1] if y > 0 else None
            above = values[y + 1] if y < ny - 1 else None
            new = update(n, x, y, left(y), right(y), values, below, above)
            dst[y, x] = new
            total = total + new
        g[x] = total

    def part_chunk(k):
        wait_y_sends(n - 1, k)
        over_rows(k, part_row, n)
    each(CHUNKS, part_chunk)

    def parts(kind, body):
        each(sets[kind][1], lambda i: body(kind, i))

    def over(kind, i, body):
        start, _, piece, _ = sets[kind]
        each(start + (i + 1) * piece, body, start + i * piece)

    def send(copy):
        return lambda kind, i: copy(kind, i).start()

    def rest_up():
        each(TAILS, lambda j: tail_up(j).start())

    def rest_dn():
        each(TAILS, lambda j: tail_dn(j).start())

    for which, choice in enumerate(choices):
        sets[:] = choice

        @pl.when(jnp.logical_and(core == which, row == 0))
        def _():
            parts(0, send(q_dn))
            parts(2, send(q_up))
            parts(1, send(q_up))
            rest_up()

            def around(kind, i):
                q_dn(kind, i).wait_recv()

                def add(x):
                    qd[x] = qd[x] + g[x]
                over(kind, i, add)
                q_dn(kind, i, qd).start()
            parts(1, around)
            parts(2, around)

        @pl.when(jnp.logical_and(core == which, row == 1))
        def _():
            parts(1, send(q_dn))
            parts(0, send(q_up))

            def both(kind, i):
                q_up(kind, i).wait_recv()
                q_dn(kind, i).wait_recv()

                def add(x):
                    own = g[x]
                    qd[x] = qd[x] + own
                    g[x] = qu[x] + own
                over(kind, i, add)
                q_up(kind, i).start()
                q_dn(kind, i, qd).start()
            parts(2, both)
            rest_up()
            rest_dn()
            parts(1, lambda kind, i: q_up(kind, i).wait_recv())
            parts(0, lambda kind, i: q_dn(kind, i).wait_recv())

        @pl.when(jnp.logical_and(core == which, row == 2))
        def _():
            parts(2, send(q_dn))
            parts(1, send(q_up))

            def both(kind, i):
                q_up(kind, i).wait_recv()

                def add(x):
                    g[x] = qu[x] + g[x]
                over(kind, i, add)
                q_up(kind, i).start()
                q_dn(kind, i).wait_recv()
                q_dn(kind, i, qd).start()
            parts(0, both)
            rest_up()
            rest_dn()
            parts(1, lambda kind, i: q_dn(kind, i).wait_recv())
            parts(2, lambda kind, i: q_up(kind, i).wait_recv())

        @pl.when(jnp.logical_and(core == which, row == 3))
        def _():
            def forward(kind, i):
                q_dn(kind, i).wait_recv()
                q_dn(kind, i, qd).start()
            parts(0, forward)
            parts(1, forward)
            rest_dn()
            parts(0, lambda kind, i: q_up(kind, i).wait_recv())
            parts(1, lambda kind, i: q_up(kind, i).wait_recv())
            parts(2, lambda kind, i: q_dn(kind, i).wait_recv())

    scale = 1.0 / (ny * rows)

    cuts = [jnp.where(core == 0, choices[0][kind][0], choices[1][kind][0]) for kind in (1, 2)]

    def end_row(x):
        low = ylo[n % 2, x]
        kind = (x >= cuts[0]).astype(jnp.int32) + (x >= cuts[1]).astype(jnp.int32)
        use_u = jnp.logical_and(has_dn, kind != row - 1)
        use_d = jnp.logical_and(has_dn, kind <= row - 1)
        sums = lax.select(use_u, qu[x], zeros) + lax.select(use_d, qd[x], zeros)
        sums = sums + inner * (src[0, x] - low)
        for y in range(ny):
            value = dst[y, x]
            if y == 0:
                value = value + 0.1 * low
            if y == ny - 1:
                value = value + 0.1 * yhi[n % 2, x]
            if y in (0, ny - 1):
                dst[y, x] = value
            sums = sums + value
            out_c[y, x] = sums * scale

    def end_chunk(k):
        wait_y_recvs(n, k)
        each((k + 1) * width, end_row, k * width)
    each(HELD, end_chunk)

    def end_tail(j):
        @pl.when(has_dn)
        def _():
            tail_up(j).wait_recv()

        @pl.when(has_up)
        def _():
            tail_dn(j).wait_recv()
        size = (nx - HELD * width) // TAILS
        each(HELD * width + (j + 1) * size, end_row, HELD * width + j * size)
    each(TAILS, end_tail)

    each(HELD, lambda k: wait_y_sends(n, k))

    @pl.when(has_up)
    def _():
        each(TAILS, lambda j: tail_up(j).wait_send())

    @pl.when(has_dn)
    def _():
        each(TAILS, lambda j: tail_dn(j).wait_send())
    wait_side_sends(n)

    for which, choice in enumerate(choices):
        sets[:] = choice
        for r in range(rows):
            @pl.when(jnp.logical_and(core == which, row == r))
            def _():
                for kind in range(3):
                    if r < rows - 1 and kind != r:
                        parts(kind, lambda kind, i: q_up(kind, i).wait_send())
                    if kind not in {0: (), 1: (0,), 2: (1,), 3: (2,)}[r]:
                        parts(kind, lambda kind, i: q_dn(kind, i).wait_send())


def write(c_ref, t_ref, out_c, out_t, sem):
    copies = []
    for i, (src, dst) in enumerate(((c_ref, out_c), (t_ref, out_t))):
        for j in range(WRITES):
            width = src.shape[1] // WRITES
            at = (slice(None), pl.ds(j * width, width)) if WRITES > src.shape[0] else (pl.ds(j * (src.shape[0] // WRITES), src.shape[0] // WRITES),)
            copies.append(pltpu.make_async_copy(src.at[at], dst.at[at], sem.at[i, j]))
    for copy in copies:
        copy.start()
    for copy in copies:
        copy.wait()


def body(tracer, crowding):
    ny, nx, nz, nl = tracer.shape
    sizes = tuple(lax.axis_size(a) for a in ("rows", "cols", "slabs"))
    shape = jax.ShapeDtypeStruct(tracer.shape, jnp.float32)
    vmem = lambda *s: pltpu.VMEM(s, jnp.float32)
    dma = pltpu.SemaphoreType.DMA
    parts = max(sum(count for _, count, _, _ in column_sets(nx, shares)) for shares in SHARES)
    sums, field = pl.pallas_call(
        functools.partial(kernel, sizes),
        out_shape=(shape, shape),
        in_specs=[pl.BlockSpec(memory_space=pltpu.HBM)] * 2,
        out_specs=[pl.BlockSpec(memory_space=pltpu.VMEM)] * 2,
        scratch_shapes=[
            vmem(ny, nx, nz, nl),
            vmem(2, nx, nz, nl), vmem(2, nx, nz, nl),
            vmem(2, ny, nz, nl), vmem(2, ny, nz, nl),
            vmem(2, ny, nx, nl), vmem(2, ny, nx, nl),
            vmem(2, ny, nx, nl), vmem(2, ny, nx, nl),
            vmem(nx, nz, nl), vmem(nx, nz, nl), vmem(nx, nz, nl),
            dma((4,)),
            dma((STEPS, CHUNKS)), dma((STEPS, CHUNKS)), dma((STEPS, CHUNKS)), dma((STEPS, CHUNKS)),
            dma((STEPS, 2)), dma((STEPS, 2)), dma((STEPS, 2)), dma((STEPS, 2)),
            dma((parts,)), dma((parts,)), dma((parts,)), dma((parts,)),
            dma((2, TAILS)), dma((2, TAILS)),
        ],
        compiler_params=pltpu.CompilerParams(
            collective_id=0, has_side_effects=True, vmem_limit_bytes=30 * 1024 * 1024),
        name="grid_steps",
    )(tracer, crowding)
    return pl.pallas_call(
        write,
        out_shape=(shape, shape),
        in_specs=[pl.BlockSpec(memory_space=pltpu.VMEM)] * 2,
        out_specs=[pl.BlockSpec(memory_space=pltpu.HBM)] * 2,
        scratch_shapes=[dma((2, WRITES))],
        compiler_params=pltpu.CompilerParams(vmem_limit_bytes=1024 * 1024),
        name="write_out",
    )(sums, field)


def solution(mesh):
    placed = P("rows", "cols", "slabs", None)
    return jax.shard_map(body, mesh=mesh, in_specs=(placed, placed), out_specs=(placed, placed), check_vma=False)
```
